32 devices in a mesh: curve: 4 (over y, core), group: 8 (over z, x).
Axes of the slice: x: 2, y: 2, z: 4, core: 2. Of those that a mesh axis runs over, the one named last changes fastest.
Arguments:
- right_side: float32 [125, 16384], P(None, ('curve', 'group')), may hold values from -6 to 6, as said below
- conductivity: float32 [16384], P(('curve', 'group')), may hold values from 0.3 to 3
- destination: int32 [16384], P(('curve', 'group')), may hold values from 0 to 16383, as said below
- neighbour: int32 [6, 16384], P(None, ('curve', 'group')), may hold values from -1 to 1023, as said below
- orientation: int32 [6, 16384], P(None, ('curve', 'group')), may hold values from 0 to 3, as said below
- send_list: int32 [2, 8192], P(None, ('curve', 'group')), may hold values from 0 to 511, as said below
Outputs:
- solution: float32 [125, 16384], P(None, ('curve', 'group'))
- residual: float32 [125, 16384], P(None, ('curve', 'group'))
The draws below stay inside these ranges and needn't reach their ends.
Inputs may be any that keep to these rules, and one draw needn't show every extreme that they name: `right_side`: custom normal-like values. `destination`: A permutation of all cells. Devices are ordered along the curve with curve slowest; every cell's new device is its old device or the one just before or after it. From each device at most 64 cells go to the next device and exactly as many come back from it; 64 is reached at some pair of neighbouring devices in every draw. `neighbour`: values below 512 are local cells of the same device. Only face 0 may name a slot from 512 to 512 + 256 - 1 (filled by the previous device from its send_list row 1), only face 1 a slot from 768 up (filled by the next device from its send_list row 0). Faces are paired: the cell across face f sees this cell across face f xor 1. -1 only at the domain boundary; the first device has no partner across its face 0 slots and the last none across face 1 slots. `orientation`: both sides of a shared face carry the same code; ignored where neighbour is -1. `send_list`: per device 256 distinct local cells in each row.
All inputs are finite; a program needn't handle non-finite values.
Results may differ from the reference program's by a relative error of at most 0.00015.
Values sent between devices are 32-bit elements; how exact they have to be, the bound alone decides.
A program may use at most 64 MiB of HBM per device.

```python
import math
import jax
import jax.numpy as jnp
from jax import lax

CELLS_DEV = 512
SIDE = 16
NODES = 5
ITERS = 2
BLOCK = 125
GHOST = 256
MOVE = 64
RANKS = 32
CELLS = 16384


def draw_right_side(key, part):
    key_rough = jax.random.fold_in(jax.random.fold_in(key, 3), 0)
    rough = jax.random.normal(key_rough, (BLOCK, CELLS), jnp.float32)
    return jnp.clip(rough, -6.0, 6.0)


def draw_destination(key, part):
    base_key = jax.random.fold_in(key, 29)
    key_swap, key_pick, key_rank, key_order = jax.random.split(base_key, 4)
    swap_counts = jax.random.randint(key_swap, (RANKS - 1,), 0, MOVE + 1).astype(jnp.int32)
    forced_at = jax.random.randint(key_pick, (), 0, RANKS - 1)
    swap_counts = swap_counts.at[forced_at].set(MOVE)
    zero_pad = jnp.zeros((1,), jnp.int32)
    to_left = jnp.concatenate([zero_pad, swap_counts])[:, None]
    to_right = jnp.concatenate([swap_counts, zero_pad])[:, None]
    local_rank = jax.vmap(lambda one_key: jax.random.permutation(one_key, CELLS_DEV))(jax.random.split(key_rank, RANKS)).astype(jnp.int32)
    old_owner = jnp.arange(RANKS, dtype=jnp.int32)[:, None]
    target = jnp.where(local_rank < to_left, old_owner - 1, jnp.where(local_rank >= CELLS_DEV - to_right, old_owner + 1, old_owner)).reshape(CELLS)
    shuffled = jax.random.permutation(key_order, CELLS).astype(jnp.int32)
    new_order = shuffled[jnp.argsort(target[shuffled], stable=True)]
    return jnp.zeros((CELLS,), jnp.int32).at[new_order].set(jnp.arange(CELLS, dtype=jnp.int32))


def mesh_arrays(key):
    base_key = jax.random.fold_in(key, 17)
    key_perm, key_code = jax.random.split(base_key)
    ghost_count = SIDE * SIDE
    layers = CELLS_DEV // ghost_count
    site_cell = jax.vmap(lambda one_key: jax.random.permutation(one_key, CELLS_DEV))(jax.random.split(key_perm, RANKS)).astype(jnp.int32)
    face_codes = jax.random.randint(key_code, (RANKS, CELLS_DEV, 3), 0, 4).astype(jnp.int32)
    site_ids = jnp.arange(CELLS_DEV, dtype=jnp.int32)
    layer_pos = (site_ids // ghost_count)[None, :]
    row_pos = (site_ids // SIDE % SIDE)[None, :]
    col_pos = (site_ids % SIDE)[None, :]
    plane_slot = row_pos * SIDE + col_pos
    rank_ids = jnp.arange(RANKS, dtype=jnp.int32)[:, None]

    def ahead_by(table, step):
        return jnp.roll(table, -step, axis=1)

    def behind_by(table, step):
        return jnp.roll(table, step, axis=1)
    face_zero = jnp.where(layer_pos > 0, behind_by(site_cell, ghost_count), jnp.where(rank_ids > 0, CELLS_DEV + plane_slot, -1))
    face_one = jnp.where(layer_pos < layers - 1, ahead_by(site_cell, ghost_count), jnp.where(rank_ids < RANKS - 1, CELLS_DEV + ghost_count + plane_slot, -1))
    face_two = jnp.where(row_pos > 0, behind_by(site_cell, SIDE), -1)
    face_three = jnp.where(row_pos < SIDE - 1, ahead_by(site_cell, SIDE), -1)
    face_four = jnp.where(col_pos > 0, behind_by(site_cell, 1), -1)
    face_five = jnp.where(col_pos < SIDE - 1, ahead_by(site_cell, 1), -1)
    code_x = face_codes[..., 0]
    code_y = face_codes[..., 1]
    code_z = face_codes[..., 2]
    previous_x = jnp.roll(jnp.roll(code_x, 1, axis=0), -(layers - 1) * ghost_count, axis=1)
    code_zero = jnp.where(layer_pos > 0, behind_by(code_x, ghost_count), previous_x)
    code_two = jnp.where(row_pos > 0, behind_by(code_y, SIDE), code_y)
    code_four = jnp.where(col_pos > 0, behind_by(code_z, 1), code_z)
    inverse = jnp.argsort(site_cell, axis=1, stable=True)
    neighbour_sites = jnp.stack([face_zero, face_one, face_two, face_three, face_four, face_five]).astype(jnp.int32)
    code_sites = jnp.stack([code_zero, code_x, code_two, code_y, code_four, code_z]).astype(jnp.int32)
    neighbour = jnp.take_along_axis(neighbour_sites, inverse[None], axis=2).reshape(6, CELLS)
    orientation = jnp.take_along_axis(code_sites, inverse[None], axis=2).reshape(6, CELLS)
    send_list = jnp.stack([site_cell[:, :ghost_count], site_cell[:, (layers - 1) * ghost_count:]]).reshape(2, RANKS * ghost_count)
    return (neighbour, orientation, send_list)


def draw_neighbour(key, part):
    return mesh_arrays(key)[0]


def draw_orientation(key, part):
    return mesh_arrays(key)[1]


def draw_send_list(key, part):
    return mesh_arrays(key)[2]


def levels(stream_key, dims, cuts, smallest, high):
    def one(dim, shards_of):
        heights = jax.random.uniform(jax.random.fold_in(jax.random.fold_in(stream_key, 6), dim), (shards_of,), jnp.float32, smallest / len(cuts), high / len(cuts))
        return jnp.repeat(jnp.exp(heights), dims[dim] // shards_of).reshape((-1,) + (1,) * (len(dims) - dim - 1))

    gain = one(*cuts[0])
    for cut in cuts[1:]:
        gain = gain * one(*cut)
    return gain


def setup_inputs(seed: int = 0) -> dict:
    arg_keys = jax.random.split(jax.random.key(seed), 7)
    right_side = draw_right_side(jax.random.fold_in(arg_keys[6], 71), 0)
    conductivity = jnp.clip(jnp.exp(math.log(3.0) - 2.3025851 * jax.random.uniform(arg_keys[1], (CELLS,), jnp.float32) ** levels(arg_keys[1], (CELLS,), ((0, 32),), -0.2, 0.2)), 0.3, 3.0)
    destination = draw_destination(jax.random.fold_in(arg_keys[6], 71), 0)
    neighbour = draw_neighbour(jax.random.fold_in(arg_keys[6], 71), 0)
    orientation = draw_orientation(jax.random.fold_in(arg_keys[6], 71), 0)
    send_list = draw_send_list(jax.random.fold_in(arg_keys[6], 71), 0)
    return {"right_side": right_side, "conductivity": conductivity, "destination": destination, "neighbour": neighbour, "orientation": orientation, "send_list": send_list}


PENALTY = 80.0
HIGHEST = lax.Precision.HIGHEST
GAUSS_POINTS = (-0.9061798459386640, -0.5384693101056831, 0.0, 0.5384693101056831, 0.9061798459386640)
GAUSS_WEIGHTS = (0.2369268850561891, 0.4786286704993665, 0.5688888888888889, 0.4786286704993665, 0.2369268850561891)


def lagrange_value(points, position, location):
    product_value = 1.0
    for other_id in range(len(points)):
        if other_id != position:
            product_value = product_value * (location - points[other_id]) / (points[position] - points[other_id])
    return product_value


def lagrange_slope(points, position, location):
    slope_sum = 0.0
    for skipped in range(len(points)):
        if skipped == position:
            continue
        addend = 1.0 / (points[position] - points[skipped])
        for other_id in range(len(points)):
            if other_id != position and other_id != skipped:
                addend = addend * (location - points[other_id]) / (points[position] - points[other_id])
        slope_sum = slope_sum + addend
    return slope_sum


def basis_tables():
    points = [0.5 * (value + 1.0) for value in GAUSS_POINTS]
    weights = [0.5 * value for value in GAUSS_WEIGHTS]
    count = len(points)
    slopes = [[lagrange_slope(points, column, points[row_id]) for column in range(count)] for row_id in range(count)]
    start_value = [lagrange_value(points, column, 0.0) for column in range(count)]
    end_value = [lagrange_value(points, column, 1.0) for column in range(count)]
    start_slope = [-lagrange_slope(points, column, 0.0) for column in range(count)]
    end_slope = [lagrange_slope(points, column, 1.0) for column in range(count)]
    listed = (weights, slopes, start_value, end_value, start_slope, end_slope)
    return tuple(jnp.asarray(table, jnp.float32) for table in listed)


def face_vectors(face_id, tables):
    if face_id % 2:
        return tables[3], tables[5]
    return tables[2], tables[4]


def face_data(block_field, conduct, face_id, tables):
    trace_vec, normal_vec = face_vectors(face_id, tables)
    axis_id = face_id // 2
    trace_value = jnp.tensordot(trace_vec, block_field, axes=([0], [axis_id]), precision=HIGHEST)
    trace_flux = conduct * jnp.tensordot(normal_vec, block_field, axes=([0], [axis_id]), precision=HIGHEST)
    return trace_value, trace_flux


def spread_back(vector, face_part, axis_id):
    bcast_shape = [1, 1, 1, 1]
    bcast_shape[axis_id] = NODES
    return vector.reshape(bcast_shape) * jnp.expand_dims(face_part, axis_id)


def volume_term(block_field, conduct, tables):
    weights, slopes = tables[0], tables[1]
    weight_3d = (weights[:, None, None] * weights[None, :, None] * weights[None, None, :])[..., None]
    result = weight_3d * block_field
    forward = ("qp,pjkc->qjkc", "qp,ipkc->iqkc", "qp,ijpc->ijqc")
    backward = ("qp,qjkc->pjkc", "qp,iqkc->ipkc", "qp,ijqc->ijpc")
    for axis_id in range(3):
        grads = jnp.einsum(forward[axis_id], slopes, block_field, precision=HIGHEST)
        result = result + jnp.einsum(backward[axis_id], slopes, weight_3d * conduct * grads, precision=HIGHEST)
    return result


def face_term(trace_value, trace_flux, conduct, other_value, other_flux, other_conduct, partner, orient_code, face_id, tables):
    weights = tables[0]
    trace_vec, normal_vec = face_vectors(face_id, tables)
    axis_id = face_id // 2
    flip_first = (orient_code % 2) == 1
    flip_second = (orient_code // 2) == 1
    other_value = jnp.where(flip_first, other_value[::-1], other_value)
    other_value = jnp.where(flip_second, other_value[:, ::-1], other_value)
    other_flux = jnp.where(flip_first, other_flux[::-1], other_flux)
    other_flux = jnp.where(flip_second, other_flux[:, ::-1], other_flux)
    outside = partner < 0
    other_value = jnp.where(outside, -trace_value, other_value)
    other_flux = jnp.where(outside, -trace_flux, other_flux)
    other_conduct = jnp.where(outside, conduct, other_conduct)
    penalty = PENALTY * jnp.maximum(conduct, other_conduct)
    trace_jump = trace_value - other_value
    mean_flux = 0.5 * (trace_flux - other_flux)
    face_weight = (weights[:, None] * weights[None, :])[:, :, None]
    first_part = spread_back(trace_vec, face_weight * (penalty * trace_jump - mean_flux), axis_id)
    return first_part + spread_back(normal_vec, face_weight * (-0.5 * conduct * trace_jump), axis_id)


def global_partners(neighbour, send_list):
    cell_ids = jnp.arange(CELLS, dtype=jnp.int32)
    owner = cell_ids // CELLS_DEV
    lower = jnp.maximum(owner - 1, 0)
    upper = jnp.minimum(owner + 1, RANKS - 1)
    left_slot = jnp.clip(neighbour - CELLS_DEV, 0, GHOST - 1)
    right_slot = jnp.clip(neighbour - CELLS_DEV - GHOST, 0, GHOST - 1)
    from_left = lower * CELLS_DEV + send_list[1][lower * GHOST + left_slot]
    from_right = upper * CELLS_DEV + send_list[0][upper * GHOST + right_slot]
    local_ids = owner * CELLS_DEV + neighbour
    joined = jnp.where(neighbour < CELLS_DEV, local_ids, jnp.where(neighbour < CELLS_DEV + GHOST, from_left, from_right))
    return jnp.where(neighbour < 0, -1, joined).astype(jnp.int32)


def operate(block_field, conduct, partners, orientation, tables):
    faces = [face_data(block_field, conduct, face_id, tables) for face_id in range(6)]
    result = volume_term(block_field, conduct, tables)
    for face_id in range(6):
        partner = partners[face_id]
        safe_idx = jnp.where(partner < 0, 0, partner)
        other_value, other_flux = faces[face_id ^ 1]
        result = result + face_term(faces[face_id][0], faces[face_id][1], conduct,
                                    other_value[:, :, safe_idx], other_flux[:, :, safe_idx], conduct[safe_idx],
                                    partner, orientation[face_id], face_id, tables)
    return result


def reference(right_side, conductivity, destination, neighbour, orientation, send_list):
    tables = basis_tables()
    placed = jnp.zeros((BLOCK, CELLS), jnp.float32).at[:, destination].set(right_side)
    conduct = jnp.zeros((CELLS,), jnp.float32).at[destination].set(conductivity)
    partners = global_partners(neighbour, send_list)
    source = placed.reshape(NODES, NODES, NODES, CELLS)
    solution = jnp.zeros_like(source)
    residual = source
    direction = source
    norm_now = jnp.sum(residual * residual)
    for step in range(ITERS):
        image = operate(direction, conduct, partners, orientation, tables)
        step_size = norm_now / jnp.sum(direction * image)
        solution = solution + step_size * direction
        residual = residual - step_size * image
        if step + 1 < ITERS:
            norm_next = jnp.sum(residual * residual)
            direction = residual + (norm_next / norm_now) * direction
            norm_now = norm_next
    return solution.reshape(BLOCK, CELLS), residual.reshape(BLOCK, CELLS)
```

```python
import functools

import jax
import jax.numpy as jnp
import numpy as np
from jax import lax
from jax.experimental import pallas as pl
from jax.experimental.pallas import tpu as pltpu
from jax.sharding import PartitionSpec as P

NODES = 5
BLOCK = 125
MOVE = 64
PENALTY = 80.0
MESH = pl.DeviceIdType.MESH
BF = jnp.bfloat16
F32 = jnp.float32

ROWS = 128
KAPPA = 125
TAG = 126
PART = 32
FACE = 2 * PART
FACE_KAPPA = 25

GAUSS_POINTS = (-0.906179845938664, -0.5384693101056831, 0.0, 0.5384693101056831, 0.906179845938664)
GAUSS_WEIGHTS = (
    0.2369268850561891,
    0.4786286704993665,
    0.5688888888888889,
    0.4786286704993665,
    0.2369268850561891,
)


def lagrange_value(points, position, location):
    out = 1.0
    for other in range(len(points)):
        if other != position:
            out = out * (location - points[other]) / (points[position] - points[other])
    return out


def lagrange_slope(points, position, location):
    total = 0.0
    for skipped in range(len(points)):
        if skipped == position:
            continue
        addend = 1.0 / (points[position] - points[skipped])
        for other in range(len(points)):
            if other != position and other != skipped:
                addend = addend * (location - points[other]) / (points[position] - points[other])
        total = total + addend
    return total


def along_axis(matrix, axis):
    five = np.eye(NODES)
    plane = np.eye(NODES * NODES)
    if axis == 0:
        return np.kron(matrix, plane)
    if axis == 1:
        return np.kron(five, np.kron(matrix, five))
    return np.kron(plane, matrix)


def split_table(table):
    high = table.astype(BF)
    low = (table - high.astype(np.float64)).astype(BF)
    return high, low


def tables():
    points = [0.5 * (value + 1.0) for value in GAUSS_POINTS]
    weights = np.array([0.5 * value for value in GAUSS_WEIGHTS])
    slopes = np.array([[lagrange_slope(points, p, points[q]) for p in range(NODES)] for q in range(NODES)])
    ends = [np.array([lagrange_value(points, p, at) for p in range(NODES)]) for at in (0.0, 1.0)]
    normals = [
        np.array([sign * lagrange_slope(points, p, at) for p in range(NODES)])
        for sign, at in ((-1.0, 0.0), (1.0, 1.0))
    ]
    cell_weight = np.kron(weights, np.kron(weights, weights))
    stiffness = np.zeros((BLOCK, BLOCK))
    for axis in range(3):
        grad = along_axis(slopes, axis)
        stiffness += grad.T @ (cell_weight[:, None] * grad)
    half = np.sqrt(0.5)
    parity_rows = np.zeros((NODES, NODES))
    for row, (a, b, sign) in enumerate(((0, 4, 1), (1, 3, 1), (2, 2, 1), (0, 4, -1), (1, 3, -1))):
        if a == b:
            parity_rows[row, a] = 1.0
        else:
            parity_rows[row, a] = half
            parity_rows[row, b] = sign * half
    parity = np.array([0, 0, 0, 1, 1])
    row_weight = weights[[0, 1, 2, 0, 1]]
    both = np.kron(parity_rows, parity_rows)
    count = NODES * NODES
    trace = np.zeros((6 * FACE, ROWS))
    for face in range(6):
        start = face * FACE
        trace[start : start + count, :BLOCK] = both @ along_axis(ends[face % 2][None, :], face // 2)
        trace[start + PART : start + PART + count, :BLOCK] = both @ along_axis(
            normals[face % 2][None, :], face // 2
        )
    lift = trace.T.copy()
    for face in range(6):
        trace[face * FACE + FACE_KAPPA, KAPPA] = 1.0
    first = np.zeros((6 * FACE + ROWS, ROWS))
    first[: 6 * FACE] = trace
    first[6 * FACE : 6 * FACE + BLOCK, :BLOCK] = stiffness
    high, low = split_table(first)
    forward = np.concatenate([high, high, low], 1)
    high, low = split_table(lift)
    backward = np.concatenate([high, low], 0)
    columns = np.zeros((ROWS, ROWS), np.float32)
    columns[:BLOCK, 0] = cell_weight
    columns[:count, 1] = np.kron(row_weight, row_weight)
    columns[:count, 2] = 2.0 * np.kron(parity, np.ones(NODES))
    columns[:count, 3] = 2.0 * np.kron(np.ones(NODES), parity)
    return forward, backward, columns


def split_two(value):
    high = value.astype(BF)
    low = (value - high.astype(F32)).astype(BF)
    return high, low


def split_three(value):
    high = value.astype(BF)
    rest = value - high.astype(F32)
    mid = rest.astype(BF)
    return high, mid, (rest - mid.astype(F32)).astype(BF)


def one_hot(left, right):
    return jnp.where(left == right, 1.0, 0.0).astype(BF)


def dot(left, right):
    return jnp.dot(left, right, preferred_element_type=F32)


def dot_last(left, right):
    return lax.dot_general(left, right, (((1,), (1,)), ((), ())), preferred_element_type=F32)


def iota(shape, dim):
    return lax.broadcasted_iota(jnp.int32, shape, dim)


def kernel(
    shape,
    rhs_ref,
    cond_ref,
    dest_ref,
    neigh_ref,
    orient_ref,
    list_ref,
    forward_ref,
    backward_ref,
    column_ref,
    x_ref,
    r_ref,
    payload,
    local_hot,
    ghost_hot,
    send_hot,
    packed,
    moved,
    halo_out,
    halo_in,
    sums,
    move_send,
    move_recv,
    halo_send,
    halo_recv,
    sum_send,
    sum_recv,
):
    curve, group = shape
    ranks = curve * group
    cells = rhs_ref.shape[1]
    ghost = list_ref.shape[1]
    me = lax.axis_index("curve") * group + lax.axis_index("group")

    def place(rank):
        return (rank // group, lax.rem(rank, group))

    def other(step):
        return place(lax.rem(me + step, ranks))

    left, right = other(ranks - 1), other(1)

    barrier = pltpu.get_barrier_semaphore()

    @pl.loop(1, ranks)
    def _(step):
        pl.semaphore_signal(barrier, inc=1, device_id=other(step), device_id_type=MESH)

    offset = dest_ref[...] - me * cells
    goes_left = offset < 0
    goes_right = offset >= cells
    slot = jnp.where(goes_left, offset + cells, jnp.where(goes_right, offset - cells, offset))
    payload[0:BLOCK, :] = rhs_ref[...]
    payload[KAPPA : KAPPA + 1, :] = cond_ref[...]
    payload[TAG : TAG + 1, :] = (slot + 1).astype(F32)
    payload[TAG + 1 : TAG + 2, :] = jnp.zeros((1, cells), F32)
    parts = jnp.concatenate(split_three(payload[...]), 0)
    row8 = iota((8, cells), 0)
    leaving = jnp.where(
        row8 == 0,
        jnp.where(goes_left, 1.0, 0.0),
        jnp.where(row8 == 1, jnp.where(goes_right, 1.0, 0.0), 0.0),
    ).astype(BF)
    triangle = jnp.where(iota((cells, cells), 0) <= iota((cells, cells), 1), 1.0, 0.0).astype(BF)
    order = dot(leaving, triangle).astype(jnp.int32) - 1
    slots = iota((MOVE, cells), 0)
    pick = jnp.concatenate(
        [
            one_hot(jnp.where(goes_left, order[0:1], -1), slots),
            one_hot(jnp.where(goes_right, order[1:2], -1), slots),
        ],
        0,
    )
    chosen = dot_last(pick, parts)
    chosen = chosen[:, :ROWS] + chosen[:, ROWS : 2 * ROWS] + chosen[:, 2 * ROWS :]
    packed[0] = chosen[:MOVE]
    packed[1] = chosen[MOVE:]

    pl.semaphore_wait(barrier, ranks - 1)

    def exchange(source, target, send_sem, recv_sem):
        copies = [
            pltpu.make_async_remote_copy(
                src_ref=source.at[side],
                dst_ref=target.at[1 - side],
                send_sem=send_sem.at[side],
                recv_sem=recv_sem.at[1 - side],
                device_id=device,
                device_id_type=MESH,
            )
            for side, device in ((0, left), (1, right))
        ]
        return copies

    moves = exchange(packed, moved, move_send, move_recv)
    for copy in moves:
        copy.start()

    stay = one_hot(iota((cells, cells), 0), offset)
    arrived = dot_last(parts, stay)
    cell_rows = iota((cells, cells), 0)
    ghost_rows = iota((ghost, cells), 0)
    for face in range(6):
        local_hot[face] = one_hot(neigh_ref[face : face + 1, :], cell_rows)
    for side in range(2):
        ghost_hot[side] = one_hot(
            neigh_ref[side : side + 1, :] - (cells + side * ghost), ghost_rows
        )
        send_hot[side] = one_hot(list_ref[side : side + 1, :], iota((cells, ghost), 0))

    for copy in moves:
        copy.wait()
    record = moved[...].reshape(2 * MOVE, ROWS)
    landing = record[:, TAG : TAG + 1].astype(jnp.int32) - 1
    record_parts = jnp.concatenate(split_three(record.T), 0)
    arrived = arrived + dot(record_parts, one_hot(landing, iota((2 * MOVE, cells), 1)))
    arrived = arrived[:ROWS] + arrived[ROWS : 2 * ROWS] + arrived[2 * ROWS :]
    rows = iota((ROWS, cells), 0)
    field = jnp.where(rows < BLOCK, arrived, 0.0)
    kappa = arrived[KAPPA : KAPPA + 1]
    cell_weight = column_ref[:, 0:1]
    face_weight = column_ref[0:PART, 1:2]
    first_odd = column_ref[0:PART, 2:3]
    second_odd = column_ref[0:PART, 3:4]

    def operate(field, turn, between):
        high, low = split_two(jnp.where(rows == KAPPA, kappa, field))
        stacked = jnp.concatenate([high, low, high], 0)

        def faces_of(first, last):
            part = dot(forward_ref[first * FACE : last * FACE, :], stacked)
            own, halves = [], []
            for index in range(last - first):
                value = part[index * FACE : index * FACE + PART]
                flux = kappa * part[index * FACE + PART : (index + 1) * FACE]
                own.append((value, flux))
                halves.append(
                    jnp.concatenate(split_two(jnp.concatenate([value, flux], 0)), 0)
                )
            return own, halves

        own, halves = faces_of(0, 2)
        for side in range(2):
            out = dot(halves[side], send_hot[side])
            halo_out[turn, side] = out[:FACE] + out[FACE:]
        copies = exchange(
            halo_out.at[turn], halo_in.at[turn], halo_send.at[turn], halo_recv.at[turn]
        )
        for copy in copies:
            copy.start()
        more_own, more_halves = faces_of(2, 6)
        own, halves = own + more_own, halves + more_halves

        def coefficients(face, near):
            value, flux = own[face]
            code = orient_ref[face : face + 1, :]
            first_bit = jnp.where(lax.rem(code, 2) == 1, 1.0, 0.0)
            second_bit = jnp.where(code >= 2, 1.0, 0.0)
            sign = (1.0 - first_odd * first_bit) * (1.0 - second_odd * second_bit)
            outside = jnp.where(neigh_ref[face : face + 1, :] < 0, 1.0, 0.0)
            near = near[:FACE] + near[FACE:]
            near_kappa = near[FACE_KAPPA : FACE_KAPPA + 1] + outside * kappa
            penalty = PENALTY * jnp.maximum(kappa, near_kappa)
            jump = value - (sign * near[:PART] - outside * value)
            mean = flux - (sign * near[PART:] - outside * flux)
            return [
                face_weight * (penalty * jump - 0.5 * mean),
                face_weight * (-0.5 * kappa * jump),
            ]

        def lifted(terms, first, last):
            high, low = split_two(jnp.concatenate(terms, 0))
            both = dot(backward_ref[:, first * FACE : last * FACE], high)
            rest = dot(backward_ref[0:ROWS, first * FACE : last * FACE], low)
            return both[:ROWS] + both[ROWS:] + rest

        terms = []
        for face in range(2, 6):
            terms += coefficients(face, dot(halves[face ^ 1], local_hot[face]))
        result = lifted(terms, 2, 6)
        stiff = dot(forward_ref[6 * FACE :, :], stacked)
        result = result + cell_weight * field + kappa * stiff
        near = [dot(halves[face ^ 1], local_hot[face]) for face in range(2)]
        between()
        for copy in copies:
            copy.wait()
        terms = []
        for face in range(2):
            received = jnp.concatenate(split_two(halo_in[turn, face]), 0)
            terms += coefficients(face, near[face] + dot(received, ghost_hot[face]))
        return result + lifted(terms, 0, 2)

    def total(value):
        part = jnp.sum(value, 0, keepdims=True)
        return jnp.sum(part, 1, keepdims=True)

    image = operate(field, 0, lambda: None)
    found = []

    def early_sums():
        found.append(total(field * field))
        found.append(total(field * image))
        found.append(total(image * image))

    second = operate(image, 1, early_sums)
    found.append(total(image * second))

    lane = iota((1, ROWS), 1)
    message = jnp.zeros((1, ROWS), F32)
    for index, value in enumerate(found):
        message = jnp.where(lane == index, value, message)
    sums[0] = message

    @pl.loop(1, ranks)
    def _(step):
        pltpu.make_async_remote_copy(
            src_ref=sums.at[0],
            dst_ref=sums.at[step],
            send_sem=sum_send,
            recv_sem=sum_recv,
            device_id=other(step),
            device_id_type=MESH,
        ).start()

    rest = sums.at[pl.ds(1, ranks - 1)]
    pltpu.make_async_copy(rest, rest, sum_send).wait()
    pltpu.make_async_copy(rest, rest, sum_recv).wait()
    summed = jnp.sum(sums[...], 0)
    s00, s01, s11, s12 = (summed[:, index : index + 1] for index in range(4))
    first_step = s00 / s01
    next_norm = s00 - 2.0 * first_step * s01 + first_step * first_step * s11
    inner = s01 - 2.0 * first_step * s11 + first_step * first_step * s12
    beta = next_norm / s00
    second_step = next_norm / (inner - beta * next_norm / first_step)
    linear = first_step + second_step * (1.0 + beta)
    square = first_step * second_step
    field, image, second = field[:BLOCK], image[:BLOCK], second[:BLOCK]
    x_ref[...] = linear * field - square * image
    r_ref[...] = field - linear * image + square * second


def body(shape, right_side, conductivity, destination, neighbour, orientation, send_list):
    cells = right_side.shape[1]
    ghost = send_list.shape[1]
    ranks = shape[0] * shape[1]
    forward, backward, columns = tables()
    vmem = pl.BlockSpec(memory_space=pltpu.VMEM)
    dma = pltpu.SemaphoreType.DMA
    return pl.pallas_call(
        functools.partial(kernel, shape),
        out_shape=(jax.ShapeDtypeStruct((BLOCK, cells), F32),) * 2,
        in_specs=[vmem] * 9,
        out_specs=(vmem, vmem),
        scratch_shapes=[
            pltpu.VMEM((ROWS, cells), F32),
            pltpu.VMEM((6, cells, cells), BF),
            pltpu.VMEM((2, ghost, cells), BF),
            pltpu.VMEM((2, cells, ghost), BF),
            pltpu.VMEM((2, MOVE, ROWS), F32),
            pltpu.VMEM((2, MOVE, ROWS), F32),
            pltpu.VMEM((2, 2, FACE, ghost), F32),
            pltpu.VMEM((2, 2, FACE, ghost), F32),
            pltpu.VMEM((ranks, 1, ROWS), F32),
            dma((2,)),
            dma((2,)),
            dma((2, 2)),
            dma((2, 2)),
            dma,
            dma,
        ],
        compiler_params=pltpu.CompilerParams(collective_id=0, has_side_effects=True),
    )(
        right_side,
        conductivity[None],
        destination[None],
        neighbour,
        orientation,
        send_list,
        jnp.asarray(forward),
        jnp.asarray(backward),
        jnp.asarray(columns),
    )


def solution(mesh):
    both = ("curve", "group")
    shape = (mesh.shape["curve"], mesh.shape["group"])
    in_specs = (P(None, both), P(both), P(both), P(None, both), P(None, both), P(None, both))
    out_specs = (P(None, both), P(None, both))
    return jax.shard_map(
        functools.partial(body, shape),
        mesh=mesh,
        in_specs=in_specs,
        out_specs=out_specs,
        check_vma=False,
    )
```

```python
import functools

import jax
import jax.numpy as jnp
import numpy as np
from jax import lax
from jax.experimental import pallas as pl
from jax.experimental.pallas import tpu as pltpu
from jax.sharding import PartitionSpec as P

NODES = 5
BLOCK = 125
MOVE = 64
PENALTY = 80.0
MESH = pl.DeviceIdType.MESH
BF = jnp.bfloat16
F32 = jnp.float32

ROWS = 128
KAPPA = 125
TAG = 126
PART = 32
FACE = 2 * PART
FACE_KAPPA = 25
FACE_TAG = 26

GAUSS_POINTS = (-0.906179845938664, -0.5384693101056831, 0.0, 0.5384693101056831, 0.906179845938664)
GAUSS_WEIGHTS = (
    0.2369268850561891,
    0.4786286704993665,
    0.5688888888888889,
    0.4786286704993665,
    0.2369268850561891,
)


def lagrange_value(points, position, location):
    out = 1.0
    for other in range(len(points)):
        if other != position:
            out = out * (location - points[other]) / (points[position] - points[other])
    return out


def lagrange_slope(points, position, location):
    total = 0.0
    for skipped in range(len(points)):
        if skipped == position:
            continue
        addend = 1.0 / (points[position] - points[skipped])
        for other in range(len(points)):
            if other != position and other != skipped:
                addend = addend * (location - points[other]) / (points[position] - points[other])
        total = total + addend
    return total


def along_axis(matrix, axis):
    five = np.eye(NODES)
    plane = np.eye(NODES * NODES)
    if axis == 0:
        return np.kron(matrix, plane)
    if axis == 1:
        return np.kron(five, np.kron(matrix, five))
    return np.kron(plane, matrix)


def split_table(table):
    high = table.astype(BF)
    low = (table - high.astype(np.float64)).astype(BF)
    return high, low


def tables():
    points = [0.5 * (value + 1.0) for value in GAUSS_POINTS]
    weights = np.array([0.5 * value for value in GAUSS_WEIGHTS])
    slopes = np.array([[lagrange_slope(points, p, points[q]) for p in range(NODES)] for q in range(NODES)])
    ends = [np.array([lagrange_value(points, p, at) for p in range(NODES)]) for at in (0.0, 1.0)]
    normals = [
        np.array([sign * lagrange_slope(points, p, at) for p in range(NODES)])
        for sign, at in ((-1.0, 0.0), (1.0, 1.0))
    ]
    cell_weight = np.kron(weights, np.kron(weights, weights))
    stiffness = np.zeros((BLOCK, BLOCK))
    for axis in range(3):
        grad = along_axis(slopes, axis)
        stiffness += grad.T @ (cell_weight[:, None] * grad)
    half = np.sqrt(0.5)
    parity_rows = np.zeros((NODES, NODES))
    for row, (a, b, sign) in enumerate(((0, 4, 1), (1, 3, 1), (2, 2, 1), (0, 4, -1), (1, 3, -1))):
        if a == b:
            parity_rows[row, a] = 1.0
        else:
            parity_rows[row, a] = half
            parity_rows[row, b] = sign * half
    parity = np.array([0, 0, 0, 1, 1])
    row_weight = weights[[0, 1, 2, 0, 1]]
    both = np.kron(parity_rows, parity_rows)
    count = NODES * NODES
    trace = np.zeros((6 * FACE, ROWS))
    for face in range(6):
        start = face * FACE
        trace[start : start + count, :BLOCK] = both @ along_axis(ends[face % 2][None, :], face // 2)
        trace[start + PART : start + PART + count, :BLOCK] = both @ along_axis(
            normals[face % 2][None, :], face // 2
        )
    lift = trace.T.copy()
    for face in range(6):
        trace[face * FACE + FACE_KAPPA, KAPPA] = 1.0
    first = np.zeros((6 * FACE + ROWS, ROWS))
    first[: 6 * FACE] = trace
    first[6 * FACE : 6 * FACE + BLOCK, :BLOCK] = stiffness
    high, low = split_table(first)
    forward = np.concatenate([high, high, low], 1)
    high, low = split_table(lift)
    backward = np.concatenate([high, low], 0)
    columns = np.zeros((ROWS, ROWS), np.float32)
    columns[:BLOCK, 0] = cell_weight
    columns[:count, 1] = np.kron(row_weight, row_weight)
    columns[:count, 2] = 2.0 * np.kron(parity, np.ones(NODES))
    columns[:count, 3] = 2.0 * np.kron(np.ones(NODES), parity)
    return forward, backward, columns


def split_two(value):
    high = value.astype(BF)
    low = (value - high.astype(F32)).astype(BF)
    return high, low


def split_three(value):
    high = value.astype(BF)
    rest = value - high.astype(F32)
    mid = rest.astype(BF)
    return high, mid, (rest - mid.astype(F32)).astype(BF)


def one_hot(left, right):
    return jnp.where(left == right, 1.0, 0.0).astype(BF)


def dot(left, right):
    return jnp.dot(left, right, preferred_element_type=F32)


def dot_last(left, right):
    return lax.dot_general(left, right, (((1,), (1,)), ((), ())), preferred_element_type=F32)


def iota(shape, dim):
    return lax.broadcasted_iota(jnp.int32, shape, dim)


def kernel(
    shape,
    rhs_hbm,
    cond_hbm,
    dest_hbm,
    neigh_hbm,
    orient_hbm,
    list_hbm,
    forward_hbm,
    backward_hbm,
    column_hbm,
    basis_hbm,
    step_ref,
    rhs_ref,
    cond_ref,
    dest_ref,
    neigh_ref,
    orient_ref,
    list_ref,
    forward_ref,
    backward_ref,
    column_ref,
    basis,
    payload,
    local_hot,
    ghost_hot,
    send_hot,
    packed,
    moved,
    far_out,
    far_in,
    halo_out,
    halo_in,
    sums,
    load_sem,
    store_sem,
    move_send,
    move_recv,
    far_send,
    far_recv,
    halo_send,
    halo_recv,
    sum_send,
    sum_recv,
):
    curve, group = shape
    ranks = curve * group
    cells = rhs_ref.shape[1]
    ghost = list_ref.shape[1]
    me = lax.axis_index("curve") * group + lax.axis_index("group")

    def place(rank):
        return (rank // group, lax.rem(rank, group))

    def other(step):
        return place(lax.rem(me + step, ranks))

    barrier = pltpu.get_barrier_semaphore()

    @pl.loop(1, ranks)
    def _(step):
        pl.semaphore_signal(barrier, inc=1, device_id=other(step), device_id_type=MESH)

    loads = [
        pltpu.make_async_copy(source, target, load_sem.at[index])
        for index, (source, target) in enumerate(
            (
                (dest_hbm, dest_ref),
                (list_hbm, list_ref),
                (cond_hbm, cond_ref),
                (rhs_hbm, rhs_ref),
                (forward_hbm, forward_ref),
                (neigh_hbm, neigh_ref),
                (orient_hbm, orient_ref),
                (column_hbm, column_ref),
                (backward_hbm, backward_ref),
            )
        )
    ]
    for load in loads:
        load.start()
    for load in loads:
        load.wait()

    def faces_of(stacked, kappa, first, last):
        part = dot(forward_ref[first * FACE : last * FACE, :], stacked)
        own, halves = [], []
        for index in range(last - first):
            value = part[index * FACE : index * FACE + PART]
            flux = kappa * part[index * FACE + PART : (index + 1) * FACE]
            own.append((value, flux))
            halves.append(jnp.concatenate(split_two(jnp.concatenate([value, flux], 0)), 0))
        return own, halves

    offset = dest_ref[...] - me * cells
    goes_left = offset < 0
    goes_right = offset >= cells
    slot = jnp.where(goes_left, offset + cells, jnp.where(goes_right, offset - cells, offset))
    payload[0:BLOCK, :] = rhs_ref[...]
    payload[KAPPA : KAPPA + 1, :] = cond_ref[...]
    payload[TAG : TAG + 1, :] = (slot + 1).astype(F32)
    payload[TAG + 1 : TAG + 2, :] = jnp.zeros((1, cells), F32)
    high, mid, low = split_three(payload[...])
    parts = jnp.concatenate([high, mid, low], 0)
    row8 = iota((8, cells), 0)
    leaving = jnp.where(
        row8 == 0,
        jnp.where(goes_left, 1.0, 0.0),
        jnp.where(row8 == 1, jnp.where(goes_right, 1.0, 0.0), 0.0),
    ).astype(BF)
    triangle = jnp.where(iota((cells, cells), 0) <= iota((cells, cells), 1), 1.0, 0.0).astype(BF)
    order = dot(leaving, triangle).astype(jnp.int32) - 1
    slots = iota((MOVE, cells), 0)
    pick = jnp.concatenate(
        [
            one_hot(jnp.where(goes_left, order[0:1], -1), slots),
            one_hot(jnp.where(goes_right, order[1:2], -1), slots),
        ],
        0,
    )
    chosen = dot_last(pick, parts)
    chosen = chosen[:, :ROWS] + chosen[:, ROWS : 2 * ROWS] + chosen[:, 2 * ROWS :]
    packed[0] = chosen[:MOVE]
    packed[1] = chosen[MOVE:]

    old_halves = faces_of(jnp.concatenate([high, mid, high], 0), cond_ref[...], 0, 2)[1]
    offset_column = jnp.broadcast_to(offset.astype(F32), (8, cells)).T[:, 0:1]
    lists = list_ref[...].astype(F32)
    face_rows = iota((FACE, ghost), 0)
    for side in range(2):
        hot = one_hot(offset_column, lists[side : side + 1, :])
        out = dot(old_halves[side], hot)
        halo_out[0, side] = jnp.where(
            face_rows == FACE_TAG, lists[side : side + 1, :], out[:FACE] + out[FACE:]
        )
    lanes = iota((2 * MOVE, ROWS), 1)
    tagged = jnp.where(lanes == FACE_TAG, chosen[:, TAG : TAG + 1], 0.0)
    leaving_low = dot_last(pick, old_halves[0]) + tagged
    leaving_high = dot_last(pick, old_halves[1]) + tagged
    far_out[0] = leaving_low[:MOVE]
    far_out[1] = leaving_high[MOVE:]

    pl.semaphore_wait(barrier, ranks - 1)

    def exchange(source, target, send_sem, recv_sem, reach):
        return [
            pltpu.make_async_remote_copy(
                src_ref=source.at[side],
                dst_ref=target.at[1 - side],
                send_sem=send_sem.at[side],
                recv_sem=recv_sem.at[1 - side],
                device_id=device,
                device_id_type=MESH,
            )
            for side, device in ((0, other(ranks - reach)), (1, other(reach)))
        ]

    moves = exchange(packed, moved, move_send, move_recv, 1)
    halos = exchange(halo_out.at[0], halo_in.at[0], halo_send.at[0], halo_recv.at[0], 1)
    fars = exchange(far_out, far_in, far_send, far_recv, 2)
    for copy in moves + fars + halos:
        copy.start()

    stay = one_hot(iota((cells, cells), 0), offset)
    arrived = dot_last(parts, stay)
    cell_rows = iota((cells, cells), 0)
    ghost_rows = iota((ghost, cells), 0)
    for face in range(6):
        local_hot[face] = one_hot(neigh_ref[face : face + 1, :], cell_rows)
    for side in range(2):
        ghost_hot[side] = one_hot(
            neigh_ref[side : side + 1, :] - (cells + side * ghost), ghost_rows
        )
        send_hot[side] = one_hot(list_ref[side : side + 1, :], iota((cells, ghost), 0))

    for copy in moves:
        copy.wait()
    record = moved[...].reshape(2 * MOVE, ROWS)
    landing = record[:, TAG : TAG + 1].astype(jnp.int32) - 1
    record_parts = jnp.concatenate(split_three(record.T), 0)
    arrived = arrived + dot(record_parts, one_hot(landing, iota((2 * MOVE, cells), 1)))
    arrived = arrived[:ROWS] + arrived[ROWS : 2 * ROWS] + arrived[2 * ROWS :]
    rows = iota((ROWS, cells), 0)
    field = jnp.where(rows < BLOCK, arrived, 0.0)
    kappa = arrived[KAPPA : KAPPA + 1]
    cell_weight = column_ref[:, 0:1]
    face_weight = column_ref[0:PART, 1:2]
    first_odd = column_ref[0:PART, 2:3]
    second_odd = column_ref[0:PART, 3:4]

    def operate(field, turn, between):
        high, low = split_two(jnp.where(rows == KAPPA, kappa, field))
        stacked = jnp.concatenate([high, low, high], 0)
        own, halves = faces_of(stacked, kappa, 0, 2)
        copies = halos + fars
        if turn:
            for side in range(2):
                out = dot(halves[side], send_hot[side])
                halo_out[turn, side] = out[:FACE] + out[FACE:]
            copies = exchange(
                halo_out.at[turn], halo_in.at[turn], halo_send.at[turn], halo_recv.at[turn], 1
            )
            for copy in copies:
                copy.start()
        more_own, more_halves = faces_of(stacked, kappa, 2, 6)
        own, halves = own + more_own, halves + more_halves

        def coefficients(face, near):
            value, flux = own[face]
            code = orient_ref[face : face + 1, :]
            first_bit = jnp.where(lax.rem(code, 2) == 1, 1.0, 0.0)
            second_bit = jnp.where(code >= 2, 1.0, 0.0)
            sign = (1.0 - first_odd * first_bit) * (1.0 - second_odd * second_bit)
            outside = jnp.where(neigh_ref[face : face + 1, :] < 0, 1.0, 0.0)
            near = near[:FACE] + near[FACE:]
            near_kappa = near[FACE_KAPPA : FACE_KAPPA + 1] + outside * kappa
            penalty = PENALTY * jnp.maximum(kappa, near_kappa)
            jump = value - (sign * near[:PART] - outside * value)
            mean = flux - (sign * near[PART:] - outside * flux)
            scaled = -0.5 * (face_weight * jump)
            return face_weight * (penalty * jump - 0.5 * mean), kappa * scaled, scaled

        def lifted(terms, first, last):
            high, low = split_two(jnp.concatenate(terms, 0))
            both = dot(backward_ref[:, first * FACE : last * FACE], high)
            rest = dot(backward_ref[0:ROWS, first * FACE : last * FACE], low)
            return both[:ROWS] + both[ROWS:] + rest

        terms = []
        for face in range(2, 6):
            terms += coefficients(face, dot(halves[face ^ 1], local_hot[face]))[:2]
        result = lifted(terms, 2, 6)
        stiff = dot(forward_ref[6 * FACE :, :], stacked)
        result = result + cell_weight * field + kappa * stiff
        near = [dot(halves[face ^ 1], local_hot[face]) for face in range(2)]
        between(result)
        for copy in copies:
            copy.wait()
        terms, energy = [], 0.0
        for face in range(2):
            ghosts = halo_in[turn, face]
            if not turn:
                gone = leaving_high[:MOVE] if face == 0 else leaving_low[MOVE:]
                wide = jnp.concatenate([far_in[face], gone], 0)
                hot = one_hot(wide[:, FACE_TAG : FACE_TAG + 1] - 1.0, ghosts[FACE_TAG : FACE_TAG + 1])
                placed = dot(wide.T.astype(BF), hot)
                ghosts = ghosts + placed[:FACE] + placed[FACE:]
            received = jnp.concatenate(split_two(ghosts), 0)
            first, second, scaled = coefficients(face, near[face] + dot(received, ghost_hot[face]))
            terms += [first, second]
            energy = energy + jnp.sum(own[face][0] * first + own[face][1] * scaled, 0, keepdims=True)
        return result, energy, lambda: lifted(terms, 0, 2)

    def down(value):
        return jnp.sum(value, 0, keepdims=True)

    def save(index, value):
        basis[index] = value
        return pltpu.make_async_copy(basis.at[index], basis_hbm.at[index], store_sem.at[index])

    stores = [save(0, field)]
    stores[0].start()
    result, _, lift = operate(field, 0, lambda result: None)
    image = result + lift()
    stores.append(save(1, image))
    stores[1].start()
    found = []

    def early_sums(result):
        found.append(down(field * field))
        found.append(down(field * image))
        found.append(down(image * image))
        found.append(down(image * result))

    result, energy, lift = operate(image, 1, early_sums)
    found[3] = found[3] + energy

    lane = iota((1, ROWS), 1)
    message = jnp.zeros((1, ROWS), F32)
    for index, value in enumerate(found):
        message = jnp.where(lane == index, jnp.sum(value, 1, keepdims=True), message)
    sums[0] = message

    @pl.loop(1, ranks)
    def _(step):
        pltpu.make_async_remote_copy(
            src_ref=sums.at[0],
            dst_ref=sums.at[step],
            send_sem=sum_send,
            recv_sem=sum_recv,
            device_id=other(step),
            device_id_type=MESH,
        ).start()

    stores.append(save(2, result + lift()))
    stores[2].start()
    rest = sums.at[pl.ds(1, ranks - 1)]
    pltpu.make_async_copy(rest, rest, sum_send).wait()
    pltpu.make_async_copy(rest, rest, sum_recv).wait()
    summed = jnp.sum(sums[...], 0)
    s00, s01, s11, s12 = (summed[:, index : index + 1] for index in range(4))
    first_step = s00 / s01
    next_norm = s00 - 2.0 * first_step * s01 + first_step * first_step * s11
    inner = s01 - 2.0 * first_step * s11 + first_step * first_step * s12
    beta = next_norm / s00
    second_step = next_norm / (inner - beta * next_norm / first_step)
    linear = first_step + second_step * (1.0 + beta)
    square = first_step * second_step
    step_ref[...] = jnp.where(iota(step_ref.shape, 0) == 0, linear, square)
    for store in stores:
        store.wait()


def body(shape, right_side, conductivity, destination, neighbour, orientation, send_list):
    cells = right_side.shape[1]
    ghost = send_list.shape[1]
    ranks = shape[0] * shape[1]
    forward, backward, columns = tables()
    vmem = pl.BlockSpec(memory_space=pltpu.VMEM)
    anywhere = pl.BlockSpec(memory_space=pl.ANY)
    dma = pltpu.SemaphoreType.DMA
    operands = (
        right_side,
        conductivity[None],
        destination[None],
        neighbour,
        orientation,
        send_list,
        jnp.asarray(forward),
        jnp.asarray(backward),
        jnp.asarray(columns),
    )
    basis, steps = pl.pallas_call(
        functools.partial(kernel, shape),
        out_shape=(
            jax.ShapeDtypeStruct((3, ROWS, cells), F32),
            jax.ShapeDtypeStruct((2, cells), F32),
        ),
        in_specs=[anywhere] * len(operands),
        out_specs=(anywhere, vmem),
        scratch_shapes=[pltpu.VMEM(item.shape, item.dtype) for item in operands]
        + [
            pltpu.VMEM((3, ROWS, cells), F32),
            pltpu.VMEM((ROWS, cells), F32),
            pltpu.VMEM((6, cells, cells), BF),
            pltpu.VMEM((2, ghost, cells), BF),
            pltpu.VMEM((2, cells, ghost), BF),
            pltpu.VMEM((2, MOVE, ROWS), F32),
            pltpu.VMEM((2, MOVE, ROWS), F32),
            pltpu.VMEM((2, MOVE, ROWS), F32),
            pltpu.VMEM((2, MOVE, ROWS), F32),
            pltpu.VMEM((2, 2, FACE, ghost), F32),
            pltpu.VMEM((2, 2, FACE, ghost), F32),
            pltpu.VMEM((ranks, 1, ROWS), F32),
            dma((len(operands),)),
            dma((3,)),
            dma((2,)),
            dma((2,)),
            dma((2,)),
            dma((2,)),
            dma((2, 2)),
            dma((2, 2)),
            dma,
            dma,
        ],
        compiler_params=pltpu.CompilerParams(collective_id=0, has_side_effects=True),
    )(*operands)
    linear, square = steps[0:1], steps[1:2]
    first, second, third = (basis[index, :BLOCK] for index in range(3))
    return linear * first - square * second, first - linear * second + square * third


def solution(mesh):
    both = ("curve", "group")
    shape = (mesh.shape["curve"], mesh.shape["group"])
    in_specs = (P(None, both), P(both), P(both), P(None, both), P(None, both), P(None, both))
    out_specs = (P(None, both), P(None, both))
    return jax.shard_map(
        functools.partial(body, shape),
        mesh=mesh,
        in_specs=in_specs,
        out_specs=out_specs,
        check_vma=False,
    )
```

```python
import functools

import jax
import jax.numpy as jnp
import numpy as np
from jax import lax
from jax.experimental import pallas as pl
from jax.experimental.pallas import tpu as pltpu
from jax.sharding import PartitionSpec as P

NODES = 5
BLOCK = 125
MOVE = 64
VMEM_LIMIT = 24 * 1024 * 1024
PENALTY = 80.0
MESH = pl.DeviceIdType.MESH
BF = jnp.bfloat16
F32 = jnp.float32

ROWS = 128
KAPPA = 125
TAG = 126
PART = 32
FACE = 2 * PART
FACE_KAPPA = 25
FACE_TAG = 26

GAUSS_POINTS = (-0.906179845938664, -0.5384693101056831, 0.0, 0.5384693101056831, 0.906179845938664)
GAUSS_WEIGHTS = (
    0.2369268850561891,
    0.4786286704993665,
    0.5688888888888889,
    0.4786286704993665,
    0.2369268850561891,
)


def lagrange_value(points, position, location):
    out = 1.0
    for other in range(len(points)):
        if other != position:
            out = out * (location - points[other]) / (points[position] - points[other])
    return out


def lagrange_slope(points, position, location):
    total = 0.0
    for skipped in range(len(points)):
        if skipped == position:
            continue
        addend = 1.0 / (points[position] - points[skipped])
        for other in range(len(points)):
            if other != position and other != skipped:
                addend = addend * (location - points[other]) / (points[position] - points[other])
        total = total + addend
    return total


def along_axis(matrix, axis):
    five = np.eye(NODES)
    plane = np.eye(NODES * NODES)
    if axis == 0:
        return np.kron(matrix, plane)
    if axis == 1:
        return np.kron(five, np.kron(matrix, five))
    return np.kron(plane, matrix)


def split_table(table):
    high = table.astype(BF)
    low = (table - high.astype(np.float64)).astype(BF)
    return high, low


def tables():
    points = [0.5 * (value + 1.0) for value in GAUSS_POINTS]
    weights = np.array([0.5 * value for value in GAUSS_WEIGHTS])
    slopes = np.array([[lagrange_slope(points, p, points[q]) for p in range(NODES)] for q in range(NODES)])
    ends = [np.array([lagrange_value(points, p, at) for p in range(NODES)]) for at in (0.0, 1.0)]
    normals = [
        np.array([sign * lagrange_slope(points, p, at) for p in range(NODES)])
        for sign, at in ((-1.0, 0.0), (1.0, 1.0))
    ]
    cell_weight = np.kron(weights, np.kron(weights, weights))
    stiffness = np.zeros((BLOCK, BLOCK))
    for axis in range(3):
        grad = along_axis(slopes, axis)
        stiffness += grad.T @ (cell_weight[:, None] * grad)
    half = np.sqrt(0.5)
    parity_rows = np.zeros((NODES, NODES))
    for row, (a, b, sign) in enumerate(((0, 4, 1), (1, 3, 1), (2, 2, 1), (0, 4, -1), (1, 3, -1))):
        if a == b:
            parity_rows[row, a] = 1.0
        else:
            parity_rows[row, a] = half
            parity_rows[row, b] = sign * half
    parity = np.array([0, 0, 0, 1, 1])
    row_weight = weights[[0, 1, 2, 0, 1]]
    both = np.kron(parity_rows, parity_rows)
    count = NODES * NODES
    trace = np.zeros((6 * FACE, ROWS))
    for face in range(6):
        start = face * FACE
        trace[start : start + count, :BLOCK] = both @ along_axis(ends[face % 2][None, :], face // 2)
        trace[start + PART : start + PART + count, :BLOCK] = both @ along_axis(
            normals[face % 2][None, :], face // 2
        )
    lift = trace.T.copy()
    for face in range(6):
        trace[face * FACE + FACE_KAPPA, KAPPA] = 1.0
    first = np.zeros((6 * FACE + ROWS, ROWS))
    first[: 6 * FACE] = trace
    first[6 * FACE : 6 * FACE + BLOCK, :BLOCK] = stiffness
    high, low = split_table(first)
    forward = np.concatenate([high, high, low], 1)
    high, low = split_table(lift)
    backward = np.concatenate([high, low], 0)
    columns = np.zeros((ROWS, ROWS), np.float32)
    columns[:BLOCK, 0] = cell_weight
    columns[:count, 1] = np.kron(row_weight, row_weight)
    columns[:count, 2] = 2.0 * np.kron(parity, np.ones(NODES))
    columns[:count, 3] = 2.0 * np.kron(np.ones(NODES), parity)
    return forward, backward, columns


def split_two(value):
    high = value.astype(BF)
    low = (value - high.astype(F32)).astype(BF)
    return high, low


def split_three(value):
    high = value.astype(BF)
    rest = value - high.astype(F32)
    mid = rest.astype(BF)
    return high, mid, (rest - mid.astype(F32)).astype(BF)


def one_hot(left, right):
    return jnp.where(left == right, 1.0, 0.0).astype(BF)


def dot(left, right):
    return jnp.dot(left, right, preferred_element_type=F32)


def dot_last(left, right):
    return lax.dot_general(left, right, (((1,), (1,)), ((), ())), preferred_element_type=F32)


def iota(shape, dim):
    return lax.broadcasted_iota(jnp.int32, shape, dim)


def kernel(
    shape,
    rhs_hbm,
    cond_hbm,
    dest_hbm,
    neigh_hbm,
    orient_hbm,
    list_hbm,
    forward_hbm,
    backward_hbm,
    column_hbm,
    basis_hbm,
    linear_ref,
    square_ref,
    rhs_ref,
    cond_ref,
    dest_ref,
    neigh_ref,
    orient_ref,
    list_ref,
    forward_ref,
    backward_ref,
    column_ref,
    basis,
    payload,
    local_hot,
    ghost_hot,
    send_hot,
    packed,
    moved,
    far_out,
    far_in,
    halo_out,
    halo_in,
    sums,
    load_sem,
    store_sem,
    move_send,
    move_recv,
    far_send,
    far_recv,
    halo_send,
    halo_recv,
    sum_send,
    sum_recv,
):
    curve, group = shape
    ranks = curve * group
    cells = rhs_ref.shape[1]
    ghost = list_ref.shape[1]
    me = lax.axis_index("curve") * group + lax.axis_index("group")

    def place(rank):
        return (rank // group, lax.rem(rank, group))

    def other(step):
        return place(lax.rem(me + step, ranks))

    barrier = pltpu.get_barrier_semaphore()

    @pl.loop(1, ranks)
    def _(step):
        pl.semaphore_signal(barrier, inc=1, device_id=other(step), device_id_type=MESH)

    loads = [
        pltpu.make_async_copy(source, target, load_sem.at[index])
        for index, (source, target) in enumerate(
            (
                (dest_hbm, dest_ref),
                (list_hbm, list_ref),
                (cond_hbm, cond_ref),
                (rhs_hbm, rhs_ref),
                (forward_hbm, forward_ref),
                (neigh_hbm, neigh_ref),
                (orient_hbm, orient_ref),
                (column_hbm, column_ref),
                (backward_hbm, backward_ref),
            )
        )
    ]
    for load in loads:
        load.start()
    for load in loads:
        load.wait()

    def faces_of(stacked, kappa, first, last):
        part = dot(forward_ref[first * FACE : last * FACE, :], stacked)
        own, halves = [], []
        for index in range(last - first):
            value = part[index * FACE : index * FACE + PART]
            flux = kappa * part[index * FACE + PART : (index + 1) * FACE]
            own.append((value, flux))
            halves.append(jnp.concatenate(split_two(jnp.concatenate([value, flux], 0)), 0))
        return own, halves

    offset = dest_ref[...] - me * cells
    goes_left = offset < 0
    goes_right = offset >= cells
    slot = jnp.where(goes_left, offset + cells, jnp.where(goes_right, offset - cells, offset))
    payload[0:BLOCK, :] = rhs_ref[...]
    payload[KAPPA : KAPPA + 1, :] = cond_ref[...]
    payload[TAG : TAG + 1, :] = (slot + 1).astype(F32)
    payload[TAG + 1 : TAG + 2, :] = jnp.zeros((1, cells), F32)
    high, mid, low = split_three(payload[...])
    parts = jnp.concatenate([high, mid, low], 0)
    row8 = iota((8, cells), 0)
    leaving = jnp.where(
        row8 == 0,
        jnp.where(goes_left, 1.0, 0.0),
        jnp.where(row8 == 1, jnp.where(goes_right, 1.0, 0.0), 0.0),
    ).astype(BF)
    triangle = jnp.where(iota((cells, cells), 0) <= iota((cells, cells), 1), 1.0, 0.0).astype(BF)
    order = dot(leaving, triangle).astype(jnp.int32) - 1
    slots = iota((MOVE, cells), 0)
    pick = jnp.concatenate(
        [
            one_hot(jnp.where(goes_left, order[0:1], -1), slots),
            one_hot(jnp.where(goes_right, order[1:2], -1), slots),
        ],
        0,
    )
    chosen = dot_last(pick, parts)
    chosen = chosen[:, :ROWS] + chosen[:, ROWS : 2 * ROWS] + chosen[:, 2 * ROWS :]
    packed[0] = chosen[:MOVE]
    packed[1] = chosen[MOVE:]

    old_halves = faces_of(jnp.concatenate([high, mid, high], 0), cond_ref[...], 0, 2)[1]
    offset_column = jnp.broadcast_to(offset.astype(F32), (8, cells)).T[:, 0:1]
    lists = list_ref[...].astype(F32)
    face_rows = iota((FACE, ghost), 0)
    for side in range(2):
        hot = one_hot(offset_column, lists[side : side + 1, :])
        out = dot(old_halves[side], hot)
        halo_out[0, side] = jnp.where(
            face_rows == FACE_TAG, lists[side : side + 1, :], out[:FACE] + out[FACE:]
        )
    lanes = iota((2 * MOVE, ROWS), 1)
    tagged = jnp.where(lanes == FACE_TAG, chosen[:, TAG : TAG + 1], 0.0)
    leaving_low = dot_last(pick, old_halves[0]) + tagged
    leaving_high = dot_last(pick, old_halves[1]) + tagged
    far_out[0] = leaving_low[:MOVE]
    far_out[1] = leaving_high[MOVE:]

    pl.semaphore_wait(barrier, ranks - 1)

    def exchange(source, target, send_sem, recv_sem, reach):
        return [
            pltpu.make_async_remote_copy(
                src_ref=source.at[side],
                dst_ref=target.at[1 - side],
                send_sem=send_sem.at[side],
                recv_sem=recv_sem.at[1 - side],
                device_id=device,
                device_id_type=MESH,
            )
            for side, device in ((0, other(ranks - reach)), (1, other(reach)))
        ]

    moves = exchange(packed, moved, move_send, move_recv, 1)
    halos = exchange(halo_out.at[0], halo_in.at[0], halo_send.at[0], halo_recv.at[0], 1)
    fars = exchange(far_out, far_in, far_send, far_recv, 2)
    for copy in moves + fars + halos:
        copy.start()

    stay = one_hot(iota((cells, cells), 0), offset)
    arrived = dot_last(parts, stay)
    cell_rows = iota((cells, cells), 0)
    ghost_rows = iota((ghost, cells), 0)
    for face in range(6):
        local_hot[face] = one_hot(neigh_ref[face : face + 1, :], cell_rows)
    for side in range(2):
        ghost_hot[side] = one_hot(
            neigh_ref[side : side + 1, :] - (cells + side * ghost), ghost_rows
        )
        send_hot[side] = one_hot(list_ref[side : side + 1, :], iota((cells, ghost), 0))

    for copy in moves:
        copy.wait()
    record = moved[...].reshape(2 * MOVE, ROWS)
    landing = record[:, TAG : TAG + 1].astype(jnp.int32) - 1
    record_parts = jnp.concatenate(split_three(record.T), 0)
    arrived = arrived + dot(record_parts, one_hot(landing, iota((2 * MOVE, cells), 1)))
    arrived = arrived[:ROWS] + arrived[ROWS : 2 * ROWS] + arrived[2 * ROWS :]
    rows = iota((ROWS, cells), 0)
    field = jnp.where(rows < BLOCK, arrived, 0.0)
    kappa = arrived[KAPPA : KAPPA + 1]
    cell_weight = column_ref[:, 0:1]
    face_weight = column_ref[0:PART, 1:2]
    first_odd = column_ref[0:PART, 2:3]
    second_odd = column_ref[0:PART, 3:4]

    def operate(field, turn, between):
        high, low = split_two(jnp.where(rows == KAPPA, kappa, field))
        stacked = jnp.concatenate([high, low, high], 0)
        own, halves = faces_of(stacked, kappa, 0, 2)
        copies = halos + fars
        if turn:
            for side in range(2):
                out = dot(halves[side], send_hot[side])
                halo_out[turn, side] = out[:FACE] + out[FACE:]
            copies = exchange(
                halo_out.at[turn], halo_in.at[turn], halo_send.at[turn], halo_recv.at[turn], 1
            )
            for copy in copies:
                copy.start()
        more_own, more_halves = faces_of(stacked, kappa, 2, 6)
        own, halves = own + more_own, halves + more_halves

        def coefficients(face, near):
            value, flux = own[face]
            code = orient_ref[face : face + 1, :]
            first_bit = jnp.where(lax.rem(code, 2) == 1, 1.0, 0.0)
            second_bit = jnp.where(code >= 2, 1.0, 0.0)
            sign = (1.0 - first_odd * first_bit) * (1.0 - second_odd * second_bit)
            outside = jnp.where(neigh_ref[face : face + 1, :] < 0, 1.0, 0.0)
            near = near[:FACE] + near[FACE:]
            near_kappa = near[FACE_KAPPA : FACE_KAPPA + 1] + outside * kappa
            penalty = PENALTY * jnp.maximum(kappa, near_kappa)
            jump = value - (sign * near[:PART] - outside * value)
            mean = flux - (sign * near[PART:] - outside * flux)
            scaled = -0.5 * (face_weight * jump)
            return face_weight * (penalty * jump - 0.5 * mean), kappa * scaled, scaled

        def lifted(terms, first, last):
            high, low = split_two(jnp.concatenate(terms, 0))
            both = dot(backward_ref[:, first * FACE : last * FACE], high)
            rest = dot(backward_ref[0:ROWS, first * FACE : last * FACE], low)
            return both[:ROWS] + both[ROWS:] + rest

        terms = []
        for face in range(2, 6):
            terms += coefficients(face, dot(halves[face ^ 1], local_hot[face]))[:2]
        result = lifted(terms, 2, 6)
        stiff = dot(forward_ref[6 * FACE :, :], stacked)
        result = result + cell_weight * field + kappa * stiff
        near = [dot(halves[face ^ 1], local_hot[face]) for face in range(2)]
        between(result)
        for copy in copies:
            copy.wait()
        terms, energy = [], 0.0
        for face in range(2):
            ghosts = halo_in[turn, face]
            if not turn:
                gone = leaving_high[:MOVE] if face == 0 else leaving_low[MOVE:]
                wide = jnp.concatenate([far_in[face], gone], 0)
                hot = one_hot(wide[:, FACE_TAG : FACE_TAG + 1] - 1.0, ghosts[FACE_TAG : FACE_TAG + 1])
                placed = dot(wide.T.astype(BF), hot)
                ghosts = ghosts + placed[:FACE] + placed[FACE:]
            received = jnp.concatenate(split_two(ghosts), 0)
            first, second, scaled = coefficients(face, near[face] + dot(received, ghost_hot[face]))
            terms += [first, second]
            energy = energy + jnp.sum(own[face][0] * first + own[face][1] * scaled, 0, keepdims=True)
        return result, energy, lambda: lifted(terms, 0, 2)

    def down(value):
        return jnp.sum(value, 0, keepdims=True)

    def save(index, value):
        basis[index] = value
        return pltpu.make_async_copy(basis.at[index], basis_hbm.at[index], store_sem.at[index])

    stores = [save(0, field)]
    stores[0].start()
    result, _, lift = operate(field, 0, lambda result: None)
    image = result + lift()
    stores.append(save(1, image))
    stores[1].start()
    found = []

    def early_sums(result):
        found.append(down(field * field))
        found.append(down(field * image))
        found.append(down(image * image))
        found.append(down(image * result))

    result, energy, lift = operate(image, 1, early_sums)
    found[3] = found[3] + energy

    lane = iota((1, ROWS), 1)
    message = jnp.zeros((1, ROWS), F32)
    for index, value in enumerate(found):
        message = jnp.where(lane == index, jnp.sum(value, 1, keepdims=True), message)
    sums[0] = message

    @pl.loop(1, ranks)
    def _(step):
        pltpu.make_async_remote_copy(
            src_ref=sums.at[0],
            dst_ref=sums.at[step],
            send_sem=sum_send,
            recv_sem=sum_recv,
            device_id=other(step),
            device_id_type=MESH,
        ).start()

    stores.append(save(2, result + lift()))
    stores[2].start()
    rest = sums.at[pl.ds(1, ranks - 1)]
    pltpu.make_async_copy(rest, rest, sum_send).wait()
    pltpu.make_async_copy(rest, rest, sum_recv).wait()
    summed = jnp.sum(sums[...], 0)
    s00, s01, s11, s12 = (summed[:, index : index + 1] for index in range(4))
    first_step = s00 / s01
    next_norm = s00 - 2.0 * first_step * s01 + first_step * first_step * s11
    inner = s01 - 2.0 * first_step * s11 + first_step * first_step * s12
    beta = next_norm / s00
    second_step = next_norm / (inner - beta * next_norm / first_step)
    linear = first_step + second_step * (1.0 + beta)
    square = first_step * second_step
    linear_ref[...] = jnp.broadcast_to(linear, (1, cells))
    square_ref[...] = jnp.broadcast_to(square, (1, cells))
    for store in stores:
        store.wait()


def body(shape, right_side, conductivity, destination, neighbour, orientation, send_list):
    cells = right_side.shape[1]
    ghost = send_list.shape[1]
    ranks = shape[0] * shape[1]
    forward, backward, columns = tables()
    vmem = pl.BlockSpec(memory_space=pltpu.VMEM)
    anywhere = pl.BlockSpec(memory_space=pl.ANY)
    dma = pltpu.SemaphoreType.DMA
    operands = (
        right_side,
        conductivity[None],
        destination[None],
        neighbour,
        orientation,
        send_list,
        jnp.asarray(forward),
        jnp.asarray(backward),
        jnp.asarray(columns),
    )
    basis, linear, square = pl.pallas_call(
        functools.partial(kernel, shape),
        out_shape=(
            jax.ShapeDtypeStruct((3, ROWS, cells), F32),
            jax.ShapeDtypeStruct((1, cells), F32),
            jax.ShapeDtypeStruct((1, cells), F32),
        ),
        in_specs=[pl.BlockSpec(memory_space=pltpu.HBM)] * len(operands),
        out_specs=(anywhere, vmem, vmem),
        scratch_shapes=[pltpu.VMEM(item.shape, item.dtype) for item in operands]
        + [
            pltpu.VMEM((3, ROWS, cells), F32),
            pltpu.VMEM((ROWS, cells), F32),
            pltpu.VMEM((6, cells, cells), BF),
            pltpu.VMEM((2, ghost, cells), BF),
            pltpu.VMEM((2, cells, ghost), BF),
            pltpu.VMEM((2, MOVE, ROWS), F32),
            pltpu.VMEM((2, MOVE, ROWS), F32),
            pltpu.VMEM((2, MOVE, ROWS), F32),
            pltpu.VMEM((2, MOVE, ROWS), F32),
            pltpu.VMEM((2, 2, FACE, ghost), F32),
            pltpu.VMEM((2, 2, FACE, ghost), F32),
            pltpu.VMEM((ranks, 1, ROWS), F32),
            dma((len(operands),)),
            dma((3,)),
            dma((2,)),
            dma((2,)),
            dma((2,)),
            dma((2,)),
            dma((2, 2)),
            dma((2, 2)),
            dma,
            dma,
        ],
        compiler_params=pltpu.CompilerParams(
            collective_id=0, has_side_effects=True, vmem_limit_bytes=VMEM_LIMIT
        ),
    )(*operands)
    first, second, third = (basis[index, :BLOCK] for index in range(3))
    return linear * first - square * second, first - linear * second + square * third


def solution(mesh):
    both = ("curve", "group")
    shape = (mesh.shape["curve"], mesh.shape["group"])
    in_specs = (P(None, both), P(both), P(both), P(None, both), P(None, both), P(None, both))
    out_specs = (P(None, both), P(None, both))
    return jax.shard_map(
        functools.partial(body, shape),
        mesh=mesh,
        in_specs=in_specs,
        out_specs=out_specs,
        check_vma=False,
    )
```

```python
import functools

import jax
import jax.numpy as jnp
import numpy as np
from jax import lax
from jax.experimental import pallas as pl
from jax.experimental.pallas import tpu as pltpu
from jax.sharding import PartitionSpec as P

NODES = 5
BLOCK = 125
MOVE = 64
UNROLLED = 64
VMEM_LIMIT = 24 * 1024 * 1024
PENALTY = 80.0
MESH = pl.DeviceIdType.MESH
BF = jnp.bfloat16
F32 = jnp.float32

ROWS = 128
KAPPA = 125
TAG = 126
PART = 32
FACE = 2 * PART
FACE_KAPPA = 25
FACE_TAG = 26
HALO = PART + 24
FACE_LAST = 27

GAUSS_POINTS = (-0.906179845938664, -0.5384693101056831, 0.0, 0.5384693101056831, 0.906179845938664)
GAUSS_WEIGHTS = (
    0.2369268850561891,
    0.4786286704993665,
    0.5688888888888889,
    0.4786286704993665,
    0.2369268850561891,
)


def lagrange_value(points, position, location):
    out = 1.0
    for other in range(len(points)):
        if other != position:
            out = out * (location - points[other]) / (points[position] - points[other])
    return out


def lagrange_slope(points, position, location):
    total = 0.0
    for skipped in range(len(points)):
        if skipped == position:
            continue
        addend = 1.0 / (points[position] - points[skipped])
        for other in range(len(points)):
            if other != position and other != skipped:
                addend = addend * (location - points[other]) / (points[position] - points[other])
        total = total + addend
    return total


def along_axis(matrix, axis):
    five = np.eye(NODES)
    plane = np.eye(NODES * NODES)
    if axis == 0:
        return np.kron(matrix, plane)
    if axis == 1:
        return np.kron(five, np.kron(matrix, five))
    return np.kron(plane, matrix)


def split_table(table):
    high = table.astype(BF)
    low = (table - high.astype(np.float64)).astype(BF)
    return high, low


def tables():
    points = [0.5 * (value + 1.0) for value in GAUSS_POINTS]
    weights = np.array([0.5 * value for value in GAUSS_WEIGHTS])
    slopes = np.array([[lagrange_slope(points, p, points[q]) for p in range(NODES)] for q in range(NODES)])
    ends = [np.array([lagrange_value(points, p, at) for p in range(NODES)]) for at in (0.0, 1.0)]
    normals = [
        np.array([sign * lagrange_slope(points, p, at) for p in range(NODES)])
        for sign, at in ((-1.0, 0.0), (1.0, 1.0))
    ]
    cell_weight = np.kron(weights, np.kron(weights, weights))
    stiffness = np.zeros((BLOCK, BLOCK))
    for axis in range(3):
        grad = along_axis(slopes, axis)
        stiffness += grad.T @ (cell_weight[:, None] * grad)
    half = np.sqrt(0.5)
    parity_rows = np.zeros((NODES, NODES))
    for row, (a, b, sign) in enumerate(((0, 4, 1), (1, 3, 1), (2, 2, 1), (0, 4, -1), (1, 3, -1))):
        if a == b:
            parity_rows[row, a] = 1.0
        else:
            parity_rows[row, a] = half
            parity_rows[row, b] = sign * half
    parity = np.array([0, 0, 0, 1, 1])
    row_weight = weights[[0, 1, 2, 0, 1]]
    both = np.kron(parity_rows, parity_rows)
    count = NODES * NODES
    trace = np.zeros((6 * FACE, ROWS))
    for face in range(6):
        start = face * FACE
        trace[start : start + count, :BLOCK] = both @ along_axis(ends[face % 2][None, :], face // 2)
        trace[start + PART : start + PART + count, :BLOCK] = both @ along_axis(
            normals[face % 2][None, :], face // 2
        )
    lift = trace.T.copy()
    for face in range(6):
        trace[face * FACE + FACE_KAPPA, KAPPA] = 1.0
    first = np.zeros((6 * FACE + ROWS, ROWS))
    first[: 6 * FACE] = trace
    first[6 * FACE : 6 * FACE + BLOCK, :BLOCK] = stiffness
    high, low = split_table(first)
    forward = np.concatenate([high, high, low], 1)
    high, low = split_table(lift)
    backward = np.concatenate([high, low], 0)
    columns = np.zeros((ROWS, ROWS), np.float32)
    columns[:BLOCK, 0] = cell_weight
    columns[:count, 1] = np.kron(row_weight, row_weight)
    columns[:count, 2] = 2.0 * np.kron(parity, np.ones(NODES))
    columns[:count, 3] = 2.0 * np.kron(np.ones(NODES), parity)
    return forward, backward, columns


def split_two(value):
    high = value.astype(BF)
    low = (value - high.astype(F32)).astype(BF)
    return high, low


def split_three(value):
    high = value.astype(BF)
    rest = value - high.astype(F32)
    mid = rest.astype(BF)
    return high, mid, (rest - mid.astype(F32)).astype(BF)


def one_hot(left, right):
    return jnp.where(left == right, 1.0, 0.0).astype(BF)


def dot(left, right):
    return jnp.dot(left, right, preferred_element_type=F32)


def dot_last(left, right):
    return lax.dot_general(left, right, (((1,), (1,)), ((), ())), preferred_element_type=F32)


def iota(shape, dim):
    return lax.broadcasted_iota(jnp.int32, shape, dim)


def kernel(
    shape,
    rhs_hbm,
    cond_hbm,
    dest_hbm,
    neigh_hbm,
    orient_hbm,
    list_hbm,
    forward_hbm,
    backward_hbm,
    column_hbm,
    basis_hbm,
    linear_ref,
    square_ref,
    rhs_ref,
    cond_ref,
    dest_ref,
    neigh_ref,
    orient_ref,
    list_ref,
    forward_ref,
    backward_ref,
    column_ref,
    basis,
    payload,
    local_hot,
    ghost_hot,
    send_hot,
    packed,
    moved,
    far_out,
    far_in,
    halo_out,
    halo_in,
    sums,
    load_sem,
    store_sem,
    move_send,
    move_recv,
    far_send,
    far_recv,
    halo_send,
    halo_recv,
    sum_send,
    sum_recv,
):
    curve, group = shape
    ranks = curve * group
    cells = rhs_ref.shape[1]
    ghost = list_ref.shape[1]
    me = lax.axis_index("curve") * group + lax.axis_index("group")

    def place(rank):
        return (rank // group, lax.rem(rank, group))

    def other(step):
        return place(lax.rem(me + step, ranks))

    barrier = pltpu.get_barrier_semaphore()

    my_curve, my_group = lax.axis_index("curve"), lax.axis_index("group")

    def for_each_other(act):
        def order(count):
            return sorted(range(count), key=lambda step: -min(step, count - step))

        for curve_step in order(curve):
            to_curve = lax.rem(my_curve + curve_step, curve)

            def one(group_step):
                to_group = lax.rem(my_group + group_step, group)
                act(curve_step * group + group_step, (to_curve, to_group))

            if ranks <= UNROLLED:
                for group_step in order(group):
                    if curve_step or group_step:
                        one(group_step)
            else:
                pl.loop(0 if curve_step else 1, group)(one)

    for_each_other(
        lambda _, device: pl.semaphore_signal(barrier, inc=1, device_id=device, device_id_type=MESH)
    )

    loads = [
        pltpu.make_async_copy(source, target, load_sem.at[index])
        for index, (source, target) in enumerate(
            (
                (dest_hbm, dest_ref),
                (list_hbm, list_ref),
                (cond_hbm, cond_ref),
                (rhs_hbm, rhs_ref),
                (forward_hbm, forward_ref),
                (neigh_hbm, neigh_ref),
                (orient_hbm, orient_ref),
                (column_hbm, column_ref),
                (backward_hbm, backward_ref),
            )
        )
    ]
    for load in loads:
        load.start()
    for load in loads[:4]:
        load.wait()

    def faces_of(stacked, kappa, first, last):
        part = dot(forward_ref[first * FACE : last * FACE, :], stacked)
        own, halves = [], []
        for index in range(last - first):
            value = part[index * FACE : index * FACE + PART]
            flux = kappa * part[index * FACE + PART : (index + 1) * FACE]
            own.append((value, flux))
            halves.append(jnp.concatenate(split_two(jnp.concatenate([value, flux], 0)), 0))
        return own, halves

    offset = dest_ref[...] - me * cells
    goes_left = offset < 0
    goes_right = offset >= cells
    slot = jnp.where(goes_left, offset + cells, jnp.where(goes_right, offset - cells, offset))
    payload[0:BLOCK, :] = rhs_ref[...]
    payload[KAPPA : KAPPA + 1, :] = cond_ref[...]
    payload[TAG : TAG + 1, :] = (slot + 1).astype(F32)
    payload[TAG + 1 : TAG + 2, :] = jnp.zeros((1, cells), F32)
    high, mid, low = split_three(payload[...])
    parts = jnp.concatenate([high, mid, low], 0)
    row8 = iota((8, cells), 0)
    leaving = jnp.where(
        row8 == 0,
        jnp.where(goes_left, 1.0, 0.0),
        jnp.where(row8 == 1, jnp.where(goes_right, 1.0, 0.0), 0.0),
    ).astype(BF)
    triangle = jnp.where(iota((cells, cells), 0) <= iota((cells, cells), 1), 1.0, 0.0).astype(BF)
    order = dot(leaving, triangle).astype(jnp.int32) - 1
    slots = iota((MOVE, cells), 0)
    pick = jnp.concatenate(
        [
            one_hot(jnp.where(goes_left, order[0:1], -1), slots),
            one_hot(jnp.where(goes_right, order[1:2], -1), slots),
        ],
        0,
    )
    chosen = dot_last(pick, parts)
    chosen = chosen[:, :ROWS] + chosen[:, ROWS : 2 * ROWS] + chosen[:, 2 * ROWS :]
    packed[0] = chosen[:MOVE]
    packed[1] = chosen[MOVE:]

    for load in loads[4:]:
        load.wait()

    old_halves = faces_of(jnp.concatenate([high, mid, high], 0), cond_ref[...], 0, 2)[1]
    offset_column = jnp.broadcast_to(offset.astype(F32), (8, cells)).T[:, 0:1]
    lists = list_ref[...].astype(F32)
    halo_rows = iota((HALO, ghost), 0)

    def shrink(out):
        out = out[:FACE] + out[FACE:]
        return jnp.where(halo_rows == FACE_LAST, out[HALO : HALO + 1], out[:HALO])

    def widen(message):
        last = message[FACE_LAST : FACE_LAST + 1]
        rest = jnp.where(iota((FACE - HALO, ghost), 0) == 0, last, 0.0)
        return jnp.concatenate([message, rest], 0)

    for side in range(2):
        hot = one_hot(offset_column, lists[side : side + 1, :])
        out = dot(old_halves[side], hot)
        halo_out[0, side] = jnp.where(
            halo_rows == FACE_TAG, lists[side : side + 1, :], shrink(out)
        )
    lanes = iota((2 * MOVE, ROWS), 1)
    tagged = jnp.where(lanes == FACE_TAG, chosen[:, TAG : TAG + 1], 0.0)
    leaving_low = dot_last(pick, old_halves[0]) + tagged
    leaving_high = dot_last(pick, old_halves[1]) + tagged
    far_out[0] = leaving_low[:MOVE]
    far_out[1] = leaving_high[MOVE:]

    pl.semaphore_wait(barrier, ranks - 1)

    def exchange(source, target, send_sem, recv_sem, reach):
        return [
            pltpu.make_async_remote_copy(
                src_ref=source.at[side],
                dst_ref=target.at[1 - side],
                send_sem=send_sem.at[side],
                recv_sem=recv_sem.at[1 - side],
                device_id=device,
                device_id_type=MESH,
            )
            for side, device in ((0, other(ranks - reach)), (1, other(reach)))
        ]

    moves = exchange(packed, moved, move_send, move_recv, 1)
    halos = exchange(halo_out.at[0], halo_in.at[0], halo_send.at[0], halo_recv.at[0], 1)
    fars = exchange(far_out, far_in, far_send, far_recv, 2)
    for copy in moves + fars + halos:
        copy.start()

    stay = one_hot(iota((cells, cells), 0), offset)
    arrived = dot_last(parts, stay)
    cell_rows = iota((cells, cells), 0)
    ghost_rows = iota((ghost, cells), 0)
    for face in range(6):
        local_hot[face] = one_hot(neigh_ref[face : face + 1, :], cell_rows)
    for side in range(2):
        ghost_hot[side] = one_hot(
            neigh_ref[side : side + 1, :] - (cells + side * ghost), ghost_rows
        )
        send_hot[side] = one_hot(list_ref[side : side + 1, :], iota((cells, ghost), 0))

    for copy in moves:
        copy.wait()
    record = moved[...].reshape(2 * MOVE, ROWS)
    landing = record[:, TAG : TAG + 1].astype(jnp.int32) - 1
    record_parts = jnp.concatenate(split_three(record.T), 0)
    arrived = arrived + dot(record_parts, one_hot(landing, iota((2 * MOVE, cells), 1)))
    arrived = arrived[:ROWS] + arrived[ROWS : 2 * ROWS] + arrived[2 * ROWS :]
    rows = iota((ROWS, cells), 0)
    field = jnp.where(rows < BLOCK, arrived, 0.0)
    kappa = arrived[KAPPA : KAPPA + 1]
    cell_weight = column_ref[:, 0:1]
    face_weight = column_ref[0:PART, 1:2]
    first_odd = column_ref[0:PART, 2:3]
    second_odd = column_ref[0:PART, 3:4]

    def operate(field, turn, between):
        high, low = split_two(jnp.where(rows == KAPPA, kappa, field))
        stacked = jnp.concatenate([high, low, high], 0)
        own, halves = faces_of(stacked, kappa, 0, 2)
        copies = halos + fars
        if turn:
            for side in range(2):
                out = dot(halves[side], send_hot[side])
                halo_out[turn, side] = shrink(out)
            copies = exchange(
                halo_out.at[turn], halo_in.at[turn], halo_send.at[turn], halo_recv.at[turn], 1
            )
            for copy in copies:
                copy.start()
        more_own, more_halves = faces_of(stacked, kappa, 2, 6)
        own, halves = own + more_own, halves + more_halves

        def coefficients(face, near):
            value, flux = own[face]
            code = orient_ref[face : face + 1, :]
            first_bit = jnp.where(lax.rem(code, 2) == 1, 1.0, 0.0)
            second_bit = jnp.where(code >= 2, 1.0, 0.0)
            sign = (1.0 - first_odd * first_bit) * (1.0 - second_odd * second_bit)
            outside = jnp.where(neigh_ref[face : face + 1, :] < 0, 1.0, 0.0)
            near = near[:FACE] + near[FACE:]
            near_kappa = near[FACE_KAPPA : FACE_KAPPA + 1] + outside * kappa
            penalty = PENALTY * jnp.maximum(kappa, near_kappa)
            jump = value - (sign * near[:PART] - outside * value)
            mean = flux - (sign * near[PART:] - outside * flux)
            scaled = -0.5 * (face_weight * jump)
            return face_weight * (penalty * jump - 0.5 * mean), kappa * scaled, scaled

        def lifted(terms, first, last):
            high, low = split_two(jnp.concatenate(terms, 0))
            both = dot(backward_ref[:, first * FACE : last * FACE], high)
            rest = dot(backward_ref[0:ROWS, first * FACE : last * FACE], low)
            return both[:ROWS] + both[ROWS:] + rest

        terms = []
        for face in range(2, 6):
            terms += coefficients(face, dot(halves[face ^ 1], local_hot[face]))[:2]
        result = lifted(terms, 2, 6)
        stiff = dot(forward_ref[6 * FACE :, :], stacked)
        result = result + cell_weight * field + kappa * stiff
        near = [dot(halves[face ^ 1], local_hot[face]) for face in range(2)]
        between(result)
        for copy in copies:
            copy.wait()
        terms, energy = [], 0.0
        for face in range(2):
            ghosts = widen(halo_in[turn, face])
            if not turn:
                gone = leaving_high[:MOVE] if face == 0 else leaving_low[MOVE:]
                wide = jnp.concatenate([far_in[face], gone], 0)
                hot = one_hot(wide[:, FACE_TAG : FACE_TAG + 1] - 1.0, ghosts[FACE_TAG : FACE_TAG + 1])
                placed = dot(wide.T.astype(BF), hot)
                ghosts = ghosts + placed[:FACE] + placed[FACE:]
            received = jnp.concatenate(split_two(ghosts), 0)
            first, second, scaled = coefficients(face, near[face] + dot(received, ghost_hot[face]))
            terms += [first, second]
            energy = energy + jnp.sum(own[face][0] * first + own[face][1] * scaled, 0, keepdims=True)
        return result, energy, lambda: lifted(terms, 0, 2)

    def down(value):
        return jnp.sum(value, 0, keepdims=True)

    def save(index, value):
        basis[index] = value
        return pltpu.make_async_copy(basis.at[index], basis_hbm.at[index], store_sem.at[index])

    stores = [save(0, field)]
    stores[0].start()
    result, _, lift = operate(field, 0, lambda result: None)
    image = result + lift()
    stores.append(save(1, image))
    stores[1].start()
    found = []

    def early_sums(result):
        found.append(down(field * field))
        found.append(down(field * image))
        found.append(down(image * image))
        found.append(down(image * result))

    result, energy, lift = operate(image, 1, early_sums)
    found[3] = found[3] + energy

    lane = iota((1, ROWS), 1)
    message = jnp.zeros((1, ROWS), F32)
    for index, value in enumerate(found):
        message = jnp.where(lane == index, jnp.sum(value, 1, keepdims=True), message)
    sums[0] = message

    for_each_other(
        lambda index, device: pltpu.make_async_remote_copy(
            src_ref=sums.at[0],
            dst_ref=sums.at[index],
            send_sem=sum_send,
            recv_sem=sum_recv,
            device_id=device,
            device_id_type=MESH,
        ).start()
    )

    stores.append(save(2, result + lift()))
    stores[2].start()
    rest = sums.at[pl.ds(1, ranks - 1)]
    pltpu.make_async_copy(rest, rest, sum_send).wait()
    pltpu.make_async_copy(rest, rest, sum_recv).wait()
    summed = jnp.sum(sums[...], 0)
    s00, s01, s11, s12 = (summed[:, index : index + 1] for index in range(4))
    first_step = s00 / s01
    next_norm = s00 - 2.0 * first_step * s01 + first_step * first_step * s11
    inner = s01 - 2.0 * first_step * s11 + first_step * first_step * s12
    beta = next_norm / s00
    second_step = next_norm / (inner - beta * next_norm / first_step)
    linear = first_step + second_step * (1.0 + beta)
    square = first_step * second_step
    linear_ref[...] = jnp.broadcast_to(linear, (1, cells))
    square_ref[...] = jnp.broadcast_to(square, (1, cells))
    for store in stores:
        store.wait()


def body(shape, right_side, conductivity, destination, neighbour, orientation, send_list):
    cells = right_side.shape[1]
    ghost = send_list.shape[1]
    ranks = shape[0] * shape[1]
    forward, backward, columns = tables()
    vmem = pl.BlockSpec(memory_space=pltpu.VMEM)
    anywhere = pl.BlockSpec(memory_space=pl.ANY)
    dma = pltpu.SemaphoreType.DMA
    operands = (
        right_side,
        conductivity[None],
        destination[None],
        neighbour,
        orientation,
        send_list,
        jnp.asarray(forward),
        jnp.asarray(backward),
        jnp.asarray(columns),
    )
    operands = tuple(pltpu.with_memory_space_constraint(item, pltpu.HBM) for item in operands)
    basis, linear, square = pl.pallas_call(
        functools.partial(kernel, shape),
        out_shape=(
            jax.ShapeDtypeStruct((3, ROWS, cells), F32),
            jax.ShapeDtypeStruct((1, cells), F32),
            jax.ShapeDtypeStruct((1, cells), F32),
        ),
        in_specs=[pl.BlockSpec(memory_space=pltpu.HBM)] * len(operands),
        out_specs=(anywhere, vmem, vmem),
        scratch_shapes=[pltpu.VMEM(item.shape, item.dtype) for item in operands]
        + [
            pltpu.VMEM((3, ROWS, cells), F32),
            pltpu.VMEM((ROWS, cells), F32),
            pltpu.VMEM((6, cells, cells), BF),
            pltpu.VMEM((2, ghost, cells), BF),
            pltpu.VMEM((2, cells, ghost), BF),
            pltpu.VMEM((2, MOVE, ROWS), F32),
            pltpu.VMEM((2, MOVE, ROWS), F32),
            pltpu.VMEM((2, MOVE, ROWS), F32),
            pltpu.VMEM((2, MOVE, ROWS), F32),
            pltpu.VMEM((2, 2, HALO, ghost), F32),
            pltpu.VMEM((2, 2, HALO, ghost), F32),
            pltpu.VMEM((ranks, 1, ROWS), F32),
            dma((len(operands),)),
            dma((3,)),
            dma((2,)),
            dma((2,)),
            dma((2,)),
            dma((2,)),
            dma((2, 2)),
            dma((2, 2)),
            dma,
            dma,
        ],
        compiler_params=pltpu.CompilerParams(
            collective_id=0, has_side_effects=True, vmem_limit_bytes=VMEM_LIMIT
        ),
    )(*operands)
    first, second, third = (basis[index, :BLOCK] for index in range(3))
    return linear * first - square * second, first - linear * second + square * third


def solution(mesh):
    both = ("curve", "group")
    shape = (mesh.shape["curve"], mesh.shape["group"])
    in_specs = (P(None, both), P(both), P(both), P(None, both), P(None, both), P(None, both))
    out_specs = (P(None, both), P(None, both))
    return jax.shard_map(
        functools.partial(body, shape),
        mesh=mesh,
        in_specs=in_specs,
        out_specs=out_specs,
        check_vma=False,
    )
```

```python
import functools

import jax
import jax.numpy as jnp
import numpy as np
from jax import lax
from jax.experimental import pallas as pl
from jax.experimental.pallas import tpu as pltpu
from jax.sharding import PartitionSpec as P

NODES = 5
BLOCK = 125
MOVE = 64
UNROLLED = 64
VMEM_LIMIT = 24 * 1024 * 1024
PENALTY = 80.0
MESH = pl.DeviceIdType.MESH
BF = jnp.bfloat16
F32 = jnp.float32

ROWS = 128
KAPPA = 125
TAG = 126
PART = 32
FACE = 2 * PART
FACE_KAPPA = 25
FACE_TAG = 26
HALO = PART + 24
FACE_LAST = 27

GAUSS_POINTS = (-0.906179845938664, -0.5384693101056831, 0.0, 0.5384693101056831, 0.906179845938664)
GAUSS_WEIGHTS = (
    0.2369268850561891,
    0.4786286704993665,
    0.5688888888888889,
    0.4786286704993665,
    0.2369268850561891,
)


def lagrange_value(points, position, location):
    out = 1.0
    for other in range(len(points)):
        if other != position:
            out = out * (location - points[other]) / (points[position] - points[other])
    return out


def lagrange_slope(points, position, location):
    total = 0.0
    for skipped in range(len(points)):
        if skipped == position:
            continue
        addend = 1.0 / (points[position] - points[skipped])
        for other in range(len(points)):
            if other != position and other != skipped:
                addend = addend * (location - points[other]) / (points[position] - points[other])
        total = total + addend
    return total


def along_axis(matrix, axis):
    five = np.eye(NODES)
    plane = np.eye(NODES * NODES)
    if axis == 0:
        return np.kron(matrix, plane)
    if axis == 1:
        return np.kron(five, np.kron(matrix, five))
    return np.kron(plane, matrix)


def split_table(table):
    high = table.astype(BF)
    low = (table - high.astype(np.float64)).astype(BF)
    return high, low


def tables():
    points = [0.5 * (value + 1.0) for value in GAUSS_POINTS]
    weights = np.array([0.5 * value for value in GAUSS_WEIGHTS])
    slopes = np.array([[lagrange_slope(points, p, points[q]) for p in range(NODES)] for q in range(NODES)])
    ends = [np.array([lagrange_value(points, p, at) for p in range(NODES)]) for at in (0.0, 1.0)]
    normals = [
        np.array([sign * lagrange_slope(points, p, at) for p in range(NODES)])
        for sign, at in ((-1.0, 0.0), (1.0, 1.0))
    ]
    cell_weight = np.kron(weights, np.kron(weights, weights))
    stiffness = np.zeros((BLOCK, BLOCK))
    for axis in range(3):
        grad = along_axis(slopes, axis)
        stiffness += grad.T @ (cell_weight[:, None] * grad)
    half = np.sqrt(0.5)
    parity_rows = np.zeros((NODES, NODES))
    for row, (a, b, sign) in enumerate(((0, 4, 1), (1, 3, 1), (2, 2, 1), (0, 4, -1), (1, 3, -1))):
        if a == b:
            parity_rows[row, a] = 1.0
        else:
            parity_rows[row, a] = half
            parity_rows[row, b] = sign * half
    parity = np.array([0, 0, 0, 1, 1])
    row_weight = weights[[0, 1, 2, 0, 1]]
    both = np.kron(parity_rows, parity_rows)
    count = NODES * NODES
    trace = np.zeros((6 * FACE, ROWS))
    for face in range(6):
        start = face * FACE
        trace[start : start + count, :BLOCK] = both @ along_axis(ends[face % 2][None, :], face // 2)
        trace[start + PART : start + PART + count, :BLOCK] = both @ along_axis(
            normals[face % 2][None, :], face // 2
        )
    lift = trace.T.copy()
    for face in range(6):
        trace[face * FACE + FACE_KAPPA, KAPPA] = 1.0
    first = np.zeros((6 * FACE + ROWS, ROWS))
    first[: 6 * FACE] = trace
    first[6 * FACE : 6 * FACE + BLOCK, :BLOCK] = stiffness
    high, low = split_table(first)
    forward = np.concatenate([high, high, low], 1)
    high, low = split_table(lift)
    backward = np.concatenate([high, low], 0)
    columns = np.zeros((ROWS, ROWS), np.float32)
    columns[:BLOCK, 0] = cell_weight
    columns[:count, 1] = np.kron(row_weight, row_weight)
    columns[:count, 2] = 2.0 * np.kron(parity, np.ones(NODES))
    columns[:count, 3] = 2.0 * np.kron(np.ones(NODES), parity)
    return forward, backward, columns


def split_two(value):
    high = value.astype(BF)
    low = (value - high.astype(F32)).astype(BF)
    return high, low


def split_three(value):
    high = value.astype(BF)
    rest = value - high.astype(F32)
    mid = rest.astype(BF)
    return high, mid, (rest - mid.astype(F32)).astype(BF)


def one_hot(left, right):
    return jnp.where(left == right, 1.0, 0.0).astype(BF)


def dot(left, right):
    return jnp.dot(left, right, preferred_element_type=F32)


def dot_last(left, right):
    return lax.dot_general(left, right, (((1,), (1,)), ((), ())), preferred_element_type=F32)


def iota(shape, dim):
    return lax.broadcasted_iota(jnp.int32, shape, dim)


def kernel(
    shape,
    rhs_hbm,
    cond_hbm,
    dest_hbm,
    neigh_hbm,
    orient_hbm,
    list_hbm,
    forward_hbm,
    backward_hbm,
    column_hbm,
    basis_hbm,
    linear_ref,
    square_ref,
    rhs_ref,
    cond_ref,
    dest_ref,
    neigh_ref,
    orient_ref,
    list_ref,
    forward_ref,
    backward_ref,
    column_ref,
    basis,
    payload,
    local_hot,
    ghost_hot,
    send_hot,
    packed,
    moved,
    far_out,
    far_in,
    halo_out,
    halo_in,
    sums,
    load_sem,
    store_sem,
    move_send,
    move_recv,
    far_send,
    far_recv,
    halo_send,
    halo_recv,
    sum_send,
    sum_recv,
):
    curve, group = shape
    ranks = curve * group
    cells = rhs_ref.shape[1]
    ghost = list_ref.shape[1]
    me = lax.axis_index("curve") * group + lax.axis_index("group")

    def place(rank):
        return (rank // group, lax.rem(rank, group))

    def other(step):
        return place(lax.rem(me + step, ranks))

    barrier = pltpu.get_barrier_semaphore()

    my_curve, my_group = lax.axis_index("curve"), lax.axis_index("group")

    def for_each_other(act):
        def order(count):
            return sorted(range(count), key=lambda step: -min(step, count - step))

        for curve_step in order(curve):
            to_curve = lax.rem(my_curve + curve_step, curve)

            def one(group_step):
                to_group = lax.rem(my_group + group_step, group)
                act(curve_step * group + group_step, (to_curve, to_group))

            if ranks <= UNROLLED:
                for group_step in order(group):
                    if curve_step or group_step:
                        one(group_step)
            else:
                pl.loop(0 if curve_step else 1, group)(one)

    for_each_other(
        lambda _, device: pl.semaphore_signal(barrier, inc=1, device_id=device, device_id_type=MESH)
    )

    loads = [
        pltpu.make_async_copy(source, target, load_sem.at[index])
        for index, (source, target) in enumerate(
            (
                (dest_hbm, dest_ref),
                (list_hbm, list_ref),
                (cond_hbm, cond_ref),
                (rhs_hbm, rhs_ref),
                (forward_hbm, forward_ref),
                (neigh_hbm, neigh_ref),
                (orient_hbm, orient_ref),
                (column_hbm, column_ref),
                (backward_hbm, backward_ref),
            )
        )
    ]
    for load in loads:
        load.start()
    for load in loads[:4]:
        load.wait()

    def faces_of(stacked, kappa, first, last):
        part = dot(forward_ref[first * FACE : last * FACE, :], stacked)
        own, halves = [], []
        for index in range(last - first):
            value = part[index * FACE : index * FACE + PART]
            flux = kappa * part[index * FACE + PART : (index + 1) * FACE]
            own.append((value, flux))
            halves.append(jnp.concatenate(split_two(jnp.concatenate([value, flux], 0)), 0))
        return own, halves

    offset = dest_ref[...] - me * cells
    goes_left = offset < 0
    goes_right = offset >= cells
    slot = jnp.where(goes_left, offset + cells, jnp.where(goes_right, offset - cells, offset))
    payload[0:BLOCK, :] = rhs_ref[...]
    payload[KAPPA : KAPPA + 1, :] = cond_ref[...]
    payload[TAG : TAG + 1, :] = (slot + 1).astype(F32)
    payload[TAG + 1 : TAG + 2, :] = jnp.zeros((1, cells), F32)
    high, mid, low = split_three(payload[...])
    parts = jnp.concatenate([high, mid, low], 0)
    row8 = iota((8, cells), 0)
    leaving = jnp.where(
        row8 == 0,
        jnp.where(goes_left, 1.0, 0.0),
        jnp.where(row8 == 1, jnp.where(goes_right, 1.0, 0.0), 0.0),
    ).astype(BF)
    triangle = jnp.where(iota((cells, cells), 0) <= iota((cells, cells), 1), 1.0, 0.0).astype(BF)
    order = dot(leaving, triangle).astype(jnp.int32) - 1
    slots = iota((MOVE, cells), 0)
    pick = jnp.concatenate(
        [
            one_hot(jnp.where(goes_left, order[0:1], -1), slots),
            one_hot(jnp.where(goes_right, order[1:2], -1), slots),
        ],
        0,
    )
    chosen = dot_last(pick, parts)
    chosen = chosen[:, :ROWS] + chosen[:, ROWS : 2 * ROWS] + chosen[:, 2 * ROWS :]
    packed[0] = chosen[:MOVE]
    packed[1] = chosen[MOVE:]

    for load in loads[4:]:
        load.wait()

    old_halves = faces_of(jnp.concatenate([high, mid, high], 0), cond_ref[...], 0, 2)[1]
    offset_column = jnp.broadcast_to(offset.astype(F32), (8, cells)).T[:, 0:1]
    lists = list_ref[...].astype(F32)
    halo_rows = iota((HALO, ghost), 0)

    def shrink(out):
        out = out[:FACE] + out[FACE:]
        return jnp.where(halo_rows == FACE_LAST, out[HALO : HALO + 1], out[:HALO])

    def widen(message):
        last = message[FACE_LAST : FACE_LAST + 1]
        rest = jnp.where(iota((FACE - HALO, ghost), 0) == 0, last, 0.0)
        return jnp.concatenate([message, rest], 0)

    for side in range(2):
        hot = one_hot(offset_column, lists[side : side + 1, :])
        out = dot(old_halves[side], hot)
        halo_out[0, side] = jnp.where(
            halo_rows == FACE_TAG, lists[side : side + 1, :], shrink(out)
        )
    lanes = iota((2 * MOVE, ROWS), 1)
    tagged = jnp.where(lanes == FACE_TAG, chosen[:, TAG : TAG + 1], 0.0)
    leaving_low = dot_last(pick, old_halves[0]) + tagged
    leaving_high = dot_last(pick, old_halves[1]) + tagged
    leaving_low = leaving_low[:, :FACE] + leaving_low[:, FACE:]
    leaving_high = leaving_high[:, :FACE] + leaving_high[:, FACE:]
    middle = MOVE // 2
    far_out[0] = jnp.concatenate([leaving_low[:middle], leaving_low[middle:MOVE]], 1)
    far_out[1] = jnp.concatenate([leaving_high[MOVE : MOVE + middle], leaving_high[MOVE + middle :]], 1)

    pl.semaphore_wait(barrier, ranks - 1)

    def exchange(source, target, send_sem, recv_sem, reach):
        return [
            pltpu.make_async_remote_copy(
                src_ref=source.at[side],
                dst_ref=target.at[1 - side],
                send_sem=send_sem.at[side],
                recv_sem=recv_sem.at[1 - side],
                device_id=device,
                device_id_type=MESH,
            )
            for side, device in ((0, other(ranks - reach)), (1, other(reach)))
        ]

    moves = exchange(packed, moved, move_send, move_recv, 1)
    halos = exchange(halo_out.at[0], halo_in.at[0], halo_send.at[0], halo_recv.at[0], 1)
    fars = exchange(far_out, far_in, far_send, far_recv, 2)
    for copy in moves + fars + halos:
        copy.start()

    stay = one_hot(iota((cells, cells), 0), offset)
    arrived = dot_last(parts, stay)
    cell_rows = iota((cells, cells), 0)
    ghost_rows = iota((ghost, cells), 0)
    for face in range(6):
        local_hot[face] = one_hot(neigh_ref[face : face + 1, :], cell_rows)
    for side in range(2):
        ghost_hot[side] = one_hot(
            neigh_ref[side : side + 1, :] - (cells + side * ghost), ghost_rows
        )
        send_hot[side] = one_hot(list_ref[side : side + 1, :], iota((cells, ghost), 0))

    for copy in moves:
        copy.wait()
    record = moved[...].reshape(2 * MOVE, ROWS)
    landing = record[:, TAG : TAG + 1].astype(jnp.int32) - 1
    record_parts = jnp.concatenate(split_three(record.T), 0)
    arrived = arrived + dot(record_parts, one_hot(landing, iota((2 * MOVE, cells), 1)))
    arrived = arrived[:ROWS] + arrived[ROWS : 2 * ROWS] + arrived[2 * ROWS :]
    rows = iota((ROWS, cells), 0)
    field = jnp.where(rows < BLOCK, arrived, 0.0)
    kappa = arrived[KAPPA : KAPPA + 1]
    cell_weight = column_ref[:, 0:1]
    face_weight = column_ref[0:PART, 1:2]
    first_odd = column_ref[0:PART, 2:3]
    second_odd = column_ref[0:PART, 3:4]

    def operate(field, turn, between):
        high, low = split_two(jnp.where(rows == KAPPA, kappa, field))
        stacked = jnp.concatenate([high, low, high], 0)
        own, halves = faces_of(stacked, kappa, 0, 2)
        copies = halos + fars
        if turn:
            for side in range(2):
                out = dot(halves[side], send_hot[side])
                halo_out[turn, side] = shrink(out)
            copies = exchange(
                halo_out.at[turn], halo_in.at[turn], halo_send.at[turn], halo_recv.at[turn], 1
            )
            for copy in copies:
                copy.start()
        more_own, more_halves = faces_of(stacked, kappa, 2, 6)
        own, halves = own + more_own, halves + more_halves

        def coefficients(face, near):
            value, flux = own[face]
            code = orient_ref[face : face + 1, :]
            first_bit = jnp.where(lax.rem(code, 2) == 1, 1.0, 0.0)
            second_bit = jnp.where(code >= 2, 1.0, 0.0)
            sign = (1.0 - first_odd * first_bit) * (1.0 - second_odd * second_bit)
            outside = jnp.where(neigh_ref[face : face + 1, :] < 0, 1.0, 0.0)
            near = near[:FACE] + near[FACE:]
            near_kappa = near[FACE_KAPPA : FACE_KAPPA + 1] + outside * kappa
            penalty = PENALTY * jnp.maximum(kappa, near_kappa)
            jump = value - (sign * near[:PART] - outside * value)
            mean = flux - (sign * near[PART:] - outside * flux)
            scaled = -0.5 * (face_weight * jump)
            return face_weight * (penalty * jump - 0.5 * mean), kappa * scaled, scaled

        def lifted(terms, first, last):
            high, low = split_two(jnp.concatenate(terms, 0))
            both = dot(backward_ref[:, first * FACE : last * FACE], high)
            rest = dot(backward_ref[0:ROWS, first * FACE : last * FACE], low)
            return both[:ROWS] + both[ROWS:] + rest

        terms = []
        for face in range(2, 6):
            terms += coefficients(face, dot(halves[face ^ 1], local_hot[face]))[:2]
        result = lifted(terms, 2, 6)
        stiff = dot(forward_ref[6 * FACE :, :], stacked)
        result = result + cell_weight * field + kappa * stiff
        near = [dot(halves[face ^ 1], local_hot[face]) for face in range(2)]
        between(result)
        for copy in copies:
            copy.wait()
        terms, energy = [], 0.0
        for face in range(2):
            ghosts = widen(halo_in[turn, face])
            if not turn:
                gone = leaving_high[:MOVE] if face == 0 else leaving_low[MOVE:]
                far = far_in[face]
                wide = jnp.concatenate([far[:, :FACE], far[:, FACE:], gone], 0)
                hot = one_hot(wide[:, FACE_TAG : FACE_TAG + 1] - 1.0, ghosts[FACE_TAG : FACE_TAG + 1])
                placed = dot(jnp.concatenate(split_two(wide.T), 0), hot)
                ghosts = ghosts + placed[:FACE] + placed[FACE:]
            received = jnp.concatenate(split_two(ghosts), 0)
            first, second, scaled = coefficients(face, near[face] + dot(received, ghost_hot[face]))
            terms += [first, second]
            energy = energy + jnp.sum(own[face][0] * first + own[face][1] * scaled, 0, keepdims=True)
        return result, energy, lambda: lifted(terms, 0, 2)

    def down(value):
        return jnp.sum(value, 0, keepdims=True)

    def across(value):
        return jnp.sum(value, 1, keepdims=True)

    def save(index, value):
        basis[index] = value
        return pltpu.make_async_copy(basis.at[index], basis_hbm.at[index], store_sem.at[index])

    stores = [save(0, field)]
    stores[0].start()
    result, _, lift = operate(field, 0, lambda result: None)
    image = result + lift()
    stores.append(save(1, image))
    stores[1].start()
    found = []

    def early_sums(result):
        found.append(across(down(field * field)))
        found.append(across(down(field * image)))
        found.append(across(down(image * image)))
        found.append(down(image * result))

    result, energy, lift = operate(image, 1, early_sums)
    found[3] = across(found[3] + energy)

    lane = iota((1, ROWS), 1)
    message = jnp.zeros((1, ROWS), F32)
    for index, value in enumerate(found):
        message = jnp.where(lane == index, value, message)
    sums[0] = message

    for_each_other(
        lambda index, device: pltpu.make_async_remote_copy(
            src_ref=sums.at[0],
            dst_ref=sums.at[index],
            send_sem=sum_send,
            recv_sem=sum_recv,
            device_id=device,
            device_id_type=MESH,
        ).start()
    )

    stores.append(save(2, result + lift()))
    stores[2].start()
    rest = sums.at[pl.ds(1, ranks - 1)]
    pltpu.make_async_copy(rest, rest, sum_send).wait()
    pltpu.make_async_copy(rest, rest, sum_recv).wait()
    summed = jnp.sum(sums[...], 0)
    s00, s01, s11, s12 = (summed[:, index : index + 1] for index in range(4))
    first_step = s00 / s01
    next_norm = s00 - 2.0 * first_step * s01 + first_step * first_step * s11
    inner = s01 - 2.0 * first_step * s11 + first_step * first_step * s12
    beta = next_norm / s00
    second_step = next_norm / (inner - beta * next_norm / first_step)
    linear = first_step + second_step * (1.0 + beta)
    square = first_step * second_step
    linear_ref[...] = jnp.broadcast_to(linear, (1, cells))
    square_ref[...] = jnp.broadcast_to(square, (1, cells))
    for store in stores:
        store.wait()


def body(shape, right_side, conductivity, destination, neighbour, orientation, send_list):
    cells = right_side.shape[1]
    ghost = send_list.shape[1]
    ranks = shape[0] * shape[1]
    forward, backward, columns = tables()
    vmem = pl.BlockSpec(memory_space=pltpu.VMEM)
    anywhere = pl.BlockSpec(memory_space=pl.ANY)
    dma = pltpu.SemaphoreType.DMA
    operands = (
        right_side,
        conductivity[None],
        destination[None],
        neighbour,
        orientation,
        send_list,
        jnp.asarray(forward),
        jnp.asarray(backward),
        jnp.asarray(columns),
    )
    operands = tuple(pltpu.with_memory_space_constraint(item, pltpu.HBM) for item in operands)
    basis, linear, square = pl.pallas_call(
        functools.partial(kernel, shape),
        out_shape=(
            jax.ShapeDtypeStruct((3, ROWS, cells), F32),
            jax.ShapeDtypeStruct((1, cells), F32),
            jax.ShapeDtypeStruct((1, cells), F32),
        ),
        in_specs=[pl.BlockSpec(memory_space=pltpu.HBM)] * len(operands),
        out_specs=(anywhere, vmem, vmem),
        scratch_shapes=[pltpu.VMEM(item.shape, item.dtype) for item in operands]
        + [
            pltpu.VMEM((3, ROWS, cells), F32),
            pltpu.VMEM((ROWS, cells), F32),
            pltpu.VMEM((6, cells, cells), BF),
            pltpu.VMEM((2, ghost, cells), BF),
            pltpu.VMEM((2, cells, ghost), BF),
            pltpu.VMEM((2, MOVE, ROWS), F32),
            pltpu.VMEM((2, MOVE, ROWS), F32),
            pltpu.VMEM((2, MOVE // 2, ROWS), F32),
            pltpu.VMEM((2, MOVE // 2, ROWS), F32),
            pltpu.VMEM((2, 2, HALO, ghost), F32),
            pltpu.VMEM((2, 2, HALO, ghost), F32),
            pltpu.VMEM((ranks, 1, ROWS), F32),
            dma((len(operands),)),
            dma((3,)),
            dma((2,)),
            dma((2,)),
            dma((2,)),
            dma((2,)),
            dma((2, 2)),
            dma((2, 2)),
            dma,
            dma,
        ],
        compiler_params=pltpu.CompilerParams(
            collective_id=0, has_side_effects=True, vmem_limit_bytes=VMEM_LIMIT
        ),
    )(*operands)
    first, second, third = (basis[index, :BLOCK] for index in range(3))
    return linear * first - square * second, first - linear * second + square * third


def solution(mesh):
    both = ("curve", "group")
    shape = (mesh.shape["curve"], mesh.shape["group"])
    in_specs = (P(None, both), P(both), P(both), P(None, both), P(None, both), P(None, both))
    out_specs = (P(None, both), P(None, both))
    return jax.shard_map(
        functools.partial(body, shape),
        mesh=mesh,
        in_specs=in_specs,
        out_specs=out_specs,
        check_vma=False,
    )
```

```python
import functools

import jax
import jax.numpy as jnp
import numpy as np
from jax import lax
from jax.experimental import pallas as pl
from jax.experimental.pallas import tpu as pltpu
from jax.sharding import PartitionSpec as P

NODES = 5
BLOCK = 125
MOVE = 64
UNROLLED = 64
VMEM_LIMIT = 24 * 1024 * 1024
PENALTY = 80.0
MESH = pl.DeviceIdType.MESH
BF = jnp.bfloat16
F32 = jnp.float32

ROWS = 128
KAPPA = 125
TAG = 126
PART = 32
FACE = 2 * PART
FACE_KAPPA = 25
FACE_TAG = 26
HALO = PART + 24
FACE_LAST = 27

GAUSS_POINTS = (-0.906179845938664, -0.5384693101056831, 0.0, 0.5384693101056831, 0.906179845938664)
GAUSS_WEIGHTS = (
    0.2369268850561891,
    0.4786286704993665,
    0.5688888888888889,
    0.4786286704993665,
    0.2369268850561891,
)


def lagrange_value(points, position, location):
    out = 1.0
    for other in range(len(points)):
        if other != position:
            out = out * (location - points[other]) / (points[position] - points[other])
    return out


def lagrange_slope(points, position, location):
    total = 0.0
    for skipped in range(len(points)):
        if skipped == position:
            continue
        addend = 1.0 / (points[position] - points[skipped])
        for other in range(len(points)):
            if other != position and other != skipped:
                addend = addend * (location - points[other]) / (points[position] - points[other])
        total = total + addend
    return total


def along_axis(matrix, axis):
    five = np.eye(NODES)
    plane = np.eye(NODES * NODES)
    if axis == 0:
        return np.kron(matrix, plane)
    if axis == 1:
        return np.kron(five, np.kron(matrix, five))
    return np.kron(plane, matrix)


def split_table(table):
    high = table.astype(BF)
    low = (table - high.astype(np.float64)).astype(BF)
    return high, low


def tables():
    points = [0.5 * (value + 1.0) for value in GAUSS_POINTS]
    weights = np.array([0.5 * value for value in GAUSS_WEIGHTS])
    slopes = np.array([[lagrange_slope(points, p, points[q]) for p in range(NODES)] for q in range(NODES)])
    ends = [np.array([lagrange_value(points, p, at) for p in range(NODES)]) for at in (0.0, 1.0)]
    normals = [
        np.array([sign * lagrange_slope(points, p, at) for p in range(NODES)])
        for sign, at in ((-1.0, 0.0), (1.0, 1.0))
    ]
    cell_weight = np.kron(weights, np.kron(weights, weights))
    stiffness = np.zeros((BLOCK, BLOCK))
    for axis in range(3):
        grad = along_axis(slopes, axis)
        stiffness += grad.T @ (cell_weight[:, None] * grad)
    half = np.sqrt(0.5)
    parity_rows = np.zeros((NODES, NODES))
    for row, (a, b, sign) in enumerate(((0, 4, 1), (1, 3, 1), (2, 2, 1), (0, 4, -1), (1, 3, -1))):
        if a == b:
            parity_rows[row, a] = 1.0
        else:
            parity_rows[row, a] = half
            parity_rows[row, b] = sign * half
    parity = np.array([0, 0, 0, 1, 1])
    row_weight = weights[[0, 1, 2, 0, 1]]
    both = np.kron(parity_rows, parity_rows)
    count = NODES * NODES
    trace = np.zeros((6 * FACE, ROWS))
    for face in range(6):
        start = face * FACE
        trace[start : start + count, :BLOCK] = both @ along_axis(ends[face % 2][None, :], face // 2)
        trace[start + PART : start + PART + count, :BLOCK] = both @ along_axis(
            normals[face % 2][None, :], face // 2
        )
    lift = trace.T.copy()
    for face in range(6):
        trace[face * FACE + FACE_KAPPA, KAPPA] = 1.0
    first = np.zeros((6 * FACE + ROWS, ROWS))
    first[: 6 * FACE] = trace
    first[6 * FACE : 6 * FACE + BLOCK, :BLOCK] = stiffness
    high, low = split_table(first)
    forward = np.concatenate([high, high, low], 1)
    high, low = split_table(lift)
    backward = np.concatenate([high, low], 0)
    columns = np.zeros((ROWS, ROWS), np.float32)
    columns[:BLOCK, 0] = cell_weight
    columns[:count, 1] = np.kron(row_weight, row_weight)
    columns[:count, 2] = 2.0 * np.kron(parity, np.ones(NODES))
    columns[:count, 3] = 2.0 * np.kron(np.ones(NODES), parity)
    return forward, backward, columns


def split_two(value):
    high = value.astype(BF)
    low = (value - high.astype(F32)).astype(BF)
    return high, low


def split_three(value):
    high = value.astype(BF)
    rest = value - high.astype(F32)
    mid = rest.astype(BF)
    return high, mid, (rest - mid.astype(F32)).astype(BF)


def one_hot(left, right):
    return jnp.where(left == right, 1.0, 0.0).astype(BF)


def dot(left, right):
    return jnp.dot(left, right, preferred_element_type=F32)


def dot_last(left, right):
    return lax.dot_general(left, right, (((1,), (1,)), ((), ())), preferred_element_type=F32)


def iota(shape, dim):
    return lax.broadcasted_iota(jnp.int32, shape, dim)


def kernel(
    shape,
    rhs_hbm,
    cond_hbm,
    dest_hbm,
    neigh_hbm,
    orient_hbm,
    list_hbm,
    forward_hbm,
    backward_hbm,
    column_hbm,
    basis_hbm,
    linear_ref,
    square_ref,
    rhs_ref,
    cond_ref,
    dest_ref,
    neigh_ref,
    orient_ref,
    list_ref,
    forward_ref,
    backward_ref,
    column_ref,
    basis,
    payload,
    local_hot,
    ghost_hot,
    send_hot,
    packed,
    moved,
    far_out,
    far_in,
    halo_out,
    halo_in,
    sums,
    load_sem,
    store_sem,
    move_send,
    move_recv,
    far_send,
    far_recv,
    halo_send,
    halo_recv,
    sum_send,
    sum_recv,
):
    curve, group = shape
    ranks = curve * group
    cells = rhs_ref.shape[1]
    ghost = list_ref.shape[1]
    me = lax.axis_index("curve") * group + lax.axis_index("group")

    def place(rank):
        return (rank // group, lax.rem(rank, group))

    def other(step):
        return place(lax.rem(me + step, ranks))

    barrier = pltpu.get_barrier_semaphore()

    my_curve, my_group = lax.axis_index("curve"), lax.axis_index("group")

    def for_each_other(act):
        def order(count):
            return sorted(range(count), key=lambda step: -min(step, count - step))

        for curve_step in order(curve):
            to_curve = lax.rem(my_curve + curve_step, curve)

            def one(group_step):
                to_group = lax.rem(my_group + group_step, group)
                act(curve_step * group + group_step, (to_curve, to_group))

            if ranks <= UNROLLED:
                for group_step in order(group):
                    if curve_step or group_step:
                        one(group_step)
            else:
                pl.loop(0 if curve_step else 1, group)(one)

    for_each_other(
        lambda _, device: pl.semaphore_signal(barrier, inc=1, device_id=device, device_id_type=MESH)
    )

    loads = [
        pltpu.make_async_copy(source, target, load_sem.at[index])
        for index, (source, target) in enumerate(
            (
                (dest_hbm, dest_ref),
                (list_hbm, list_ref),
                (cond_hbm, cond_ref),
                (rhs_hbm, rhs_ref),
                (forward_hbm, forward_ref),
                (neigh_hbm, neigh_ref),
                (orient_hbm, orient_ref),
                (column_hbm, column_ref),
                (backward_hbm, backward_ref),
            )
        )
    ]
    for load in loads:
        load.start()
    for load in loads[:4]:
        load.wait()

    def faces_of(stacked, kappa, first, last):
        part = dot(forward_ref[first * FACE : last * FACE, :], stacked)
        own, halves = [], []
        for index in range(last - first):
            value = part[index * FACE : index * FACE + PART]
            flux = kappa * part[index * FACE + PART : (index + 1) * FACE]
            own.append((value, flux))
            halves.append(jnp.concatenate(split_two(jnp.concatenate([value, flux], 0)), 0))
        return own, halves

    offset = dest_ref[...] - me * cells
    goes_left = offset < 0
    goes_right = offset >= cells
    slot = jnp.where(goes_left, offset + cells, jnp.where(goes_right, offset - cells, offset))
    payload[0:BLOCK, :] = rhs_ref[...]
    payload[KAPPA : KAPPA + 1, :] = cond_ref[...]
    payload[TAG : TAG + 1, :] = (slot + 1).astype(F32)
    payload[TAG + 1 : TAG + 2, :] = jnp.zeros((1, cells), F32)
    high, mid, low = split_three(payload[...])
    parts = jnp.concatenate([high, mid, low], 0)
    row8 = iota((8, cells), 0)
    leaving = jnp.where(
        row8 == 0,
        jnp.where(goes_left, 1.0, 0.0),
        jnp.where(row8 == 1, jnp.where(goes_right, 1.0, 0.0), 0.0),
    ).astype(BF)
    triangle = jnp.where(iota((cells, cells), 0) <= iota((cells, cells), 1), 1.0, 0.0).astype(BF)
    order = dot(leaving, triangle).astype(jnp.int32) - 1
    slots = iota((MOVE, cells), 0)
    pick = jnp.concatenate(
        [
            one_hot(jnp.where(goes_left, order[0:1], -1), slots),
            one_hot(jnp.where(goes_right, order[1:2], -1), slots),
        ],
        0,
    )
    chosen = dot_last(pick, parts)
    chosen = chosen[:, :ROWS] + chosen[:, ROWS : 2 * ROWS] + chosen[:, 2 * ROWS :]
    packed[0] = chosen[:MOVE]
    packed[1] = chosen[MOVE:]

    pl.semaphore_wait(barrier, ranks - 1)

    def exchange(source, target, send_sem, recv_sem, reach):
        return [
            pltpu.make_async_remote_copy(
                src_ref=source.at[side],
                dst_ref=target.at[1 - side],
                send_sem=send_sem.at[side],
                recv_sem=recv_sem.at[1 - side],
                device_id=device,
                device_id_type=MESH,
            )
            for side, device in ((0, other(ranks - reach)), (1, other(reach)))
        ]

    moves = exchange(packed, moved, move_send, move_recv, 1)
    for copy in moves:
        copy.start()

    for load in loads[4:]:
        load.wait()

    old_halves = faces_of(jnp.concatenate([high, mid, high], 0), cond_ref[...], 0, 2)[1]
    offset_column = jnp.broadcast_to(offset.astype(F32), (8, cells)).T[:, 0:1]
    lists = list_ref[...].astype(F32)
    halo_rows = iota((HALO, ghost), 0)

    def shrink(out):
        out = out[:FACE] + out[FACE:]
        return jnp.where(halo_rows == FACE_LAST, out[HALO : HALO + 1], out[:HALO])

    def widen(message):
        last = message[FACE_LAST : FACE_LAST + 1]
        rest = jnp.where(iota((FACE - HALO, ghost), 0) == 0, last, 0.0)
        return jnp.concatenate([message, rest], 0)

    for side in range(2):
        hot = one_hot(offset_column, lists[side : side + 1, :])
        out = dot(old_halves[side], hot)
        halo_out[0, side] = jnp.where(
            halo_rows == FACE_TAG, lists[side : side + 1, :], shrink(out)
        )
    lanes = iota((2 * MOVE, ROWS), 1)
    tagged = jnp.where(lanes == FACE_TAG, chosen[:, TAG : TAG + 1], 0.0)
    leaving_low = dot_last(pick, old_halves[0]) + tagged
    leaving_high = dot_last(pick, old_halves[1]) + tagged
    leaving_low = leaving_low[:, :FACE] + leaving_low[:, FACE:]
    leaving_high = leaving_high[:, :FACE] + leaving_high[:, FACE:]
    middle = MOVE // 2
    far_out[0] = jnp.concatenate([leaving_low[:middle], leaving_low[middle:MOVE]], 1)
    far_out[1] = jnp.concatenate([leaving_high[MOVE : MOVE + middle], leaving_high[MOVE + middle :]], 1)

    halos = exchange(halo_out.at[0], halo_in.at[0], halo_send.at[0], halo_recv.at[0], 1)
    fars = exchange(far_out, far_in, far_send, far_recv, 2)
    for copy in fars + halos:
        copy.start()

    stay = one_hot(iota((cells, cells), 0), offset)
    arrived = dot_last(parts, stay)
    cell_rows = iota((cells, cells), 0)
    ghost_rows = iota((ghost, cells), 0)
    for face in range(6):
        local_hot[face] = one_hot(neigh_ref[face : face + 1, :], cell_rows)
    for side in range(2):
        ghost_hot[side] = one_hot(
            neigh_ref[side : side + 1, :] - (cells + side * ghost), ghost_rows
        )
        send_hot[side] = one_hot(list_ref[side : side + 1, :], iota((cells, ghost), 0))

    for copy in moves:
        copy.wait()
    record = moved[...].reshape(2 * MOVE, ROWS)
    landing = record[:, TAG : TAG + 1].astype(jnp.int32) - 1
    record_parts = jnp.concatenate(split_three(record.T), 0)
    arrived = arrived + dot(record_parts, one_hot(landing, iota((2 * MOVE, cells), 1)))
    arrived = arrived[:ROWS] + arrived[ROWS : 2 * ROWS] + arrived[2 * ROWS :]
    rows = iota((ROWS, cells), 0)
    field = jnp.where(rows < BLOCK, arrived, 0.0)
    kappa = arrived[KAPPA : KAPPA + 1]
    cell_weight = column_ref[:, 0:1]
    face_weight = column_ref[0:PART, 1:2]
    first_odd = column_ref[0:PART, 2:3]
    second_odd = column_ref[0:PART, 3:4]

    def operate(field, turn, between):
        high, low = split_two(jnp.where(rows == KAPPA, kappa, field))
        stacked = jnp.concatenate([high, low, high], 0)
        own, halves = faces_of(stacked, kappa, 0, 2)
        copies = halos + fars
        if turn:
            for side in range(2):
                out = dot(halves[side], send_hot[side])
                halo_out[turn, side] = shrink(out)
            copies = exchange(
                halo_out.at[turn], halo_in.at[turn], halo_send.at[turn], halo_recv.at[turn], 1
            )
            for copy in copies:
                copy.start()
        more_own, more_halves = faces_of(stacked, kappa, 2, 6)
        own, halves = own + more_own, halves + more_halves

        def coefficients(face, near):
            value, flux = own[face]
            code = orient_ref[face : face + 1, :]
            first_bit = jnp.where(lax.rem(code, 2) == 1, 1.0, 0.0)
            second_bit = jnp.where(code >= 2, 1.0, 0.0)
            sign = (1.0 - first_odd * first_bit) * (1.0 - second_odd * second_bit)
            outside = jnp.where(neigh_ref[face : face + 1, :] < 0, 1.0, 0.0)
            near = near[:FACE] + near[FACE:]
            near_kappa = near[FACE_KAPPA : FACE_KAPPA + 1] + outside * kappa
            penalty = PENALTY * jnp.maximum(kappa, near_kappa)
            jump = value - (sign * near[:PART] - outside * value)
            mean = flux - (sign * near[PART:] - outside * flux)
            scaled = -0.5 * (face_weight * jump)
            return face_weight * (penalty * jump - 0.5 * mean), kappa * scaled, scaled

        def lifted(terms, first, last):
            high, low = split_two(jnp.concatenate(terms, 0))
            both = dot(backward_ref[:, first * FACE : last * FACE], high)
            rest = dot(backward_ref[0:ROWS, first * FACE : last * FACE], low)
            return both[:ROWS] + both[ROWS:] + rest

        terms = []
        for face in range(2, 6):
            terms += coefficients(face, dot(halves[face ^ 1], local_hot[face]))[:2]
        result = lifted(terms, 2, 6)
        stiff = dot(forward_ref[6 * FACE :, :], stacked)
        result = result + cell_weight * field + kappa * stiff
        near = [dot(halves[face ^ 1], local_hot[face]) for face in range(2)]
        between(result)
        for copy in copies:
            copy.wait()
        terms, energy = [], 0.0
        for face in range(2):
            ghosts = widen(halo_in[turn, face])
            if not turn:
                gone = leaving_high[:MOVE] if face == 0 else leaving_low[MOVE:]
                far = far_in[face]
                wide = jnp.concatenate([far[:, :FACE], far[:, FACE:], gone], 0)
                hot = one_hot(wide[:, FACE_TAG : FACE_TAG + 1] - 1.0, ghosts[FACE_TAG : FACE_TAG + 1])
                placed = dot(jnp.concatenate(split_two(wide.T), 0), hot)
                ghosts = ghosts + placed[:FACE] + placed[FACE:]
            received = jnp.concatenate(split_two(ghosts), 0)
            first, second, scaled = coefficients(face, near[face] + dot(received, ghost_hot[face]))
            terms += [first, second]
            energy = energy + jnp.sum(own[face][0] * first + own[face][1] * scaled, 0, keepdims=True)
        return result, energy, lambda: lifted(terms, 0, 2)

    def down(value):
        return jnp.sum(value, 0, keepdims=True)

    def across(value):
        return jnp.sum(value, 1, keepdims=True)

    def save(index, value):
        basis[index] = value
        return pltpu.make_async_copy(basis.at[index], basis_hbm.at[index], store_sem.at[index])

    stores = [save(0, field)]
    stores[0].start()
    result, _, lift = operate(field, 0, lambda result: None)
    image = result + lift()
    stores.append(save(1, image))
    stores[1].start()
    found = []

    def early_sums(result):
        found.append(across(down(field * field)))
        found.append(across(down(field * image)))
        found.append(across(down(image * image)))
        found.append(down(image * result))

    result, energy, lift = operate(image, 1, early_sums)
    found[3] = across(found[3] + energy)

    lane = iota((1, ROWS), 1)
    message = jnp.zeros((1, ROWS), F32)
    for index, value in enumerate(found):
        message = jnp.where(lane == index, value, message)
    sums[0] = message

    for_each_other(
        lambda index, device: pltpu.make_async_remote_copy(
            src_ref=sums.at[0],
            dst_ref=sums.at[index],
            send_sem=sum_send,
            recv_sem=sum_recv,
            device_id=device,
            device_id_type=MESH,
        ).start()
    )

    stores.append(save(2, result + lift()))
    stores[2].start()
    rest = sums.at[pl.ds(1, ranks - 1)]
    pltpu.make_async_copy(rest, rest, sum_send).wait()
    pltpu.make_async_copy(rest, rest, sum_recv).wait()
    summed = jnp.sum(sums[...], 0)
    s00, s01, s11, s12 = (summed[:, index : index + 1] for index in range(4))
    first_step = s00 / s01
    next_norm = s00 - 2.0 * first_step * s01 + first_step * first_step * s11
    inner = s01 - 2.0 * first_step * s11 + first_step * first_step * s12
    beta = next_norm / s00
    second_step = next_norm / (inner - beta * next_norm / first_step)
    linear = first_step + second_step * (1.0 + beta)
    square = first_step * second_step
    linear_ref[...] = jnp.broadcast_to(linear, (1, cells))
    square_ref[...] = jnp.broadcast_to(square, (1, cells))
    for store in stores:
        store.wait()


def body(shape, right_side, conductivity, destination, neighbour, orientation, send_list):
    cells = right_side.shape[1]
    ghost = send_list.shape[1]
    ranks = shape[0] * shape[1]
    forward, backward, columns = tables()
    vmem = pl.BlockSpec(memory_space=pltpu.VMEM)
    anywhere = pl.BlockSpec(memory_space=pl.ANY)
    dma = pltpu.SemaphoreType.DMA
    operands = (
        right_side,
        conductivity[None],
        destination[None],
        neighbour,
        orientation,
        send_list,
        jnp.asarray(forward),
        jnp.asarray(backward),
        jnp.asarray(columns),
    )
    operands = tuple(pltpu.with_memory_space_constraint(item, pltpu.HBM) for item in operands)
    basis, linear, square = pl.pallas_call(
        functools.partial(kernel, shape),
        out_shape=(
            jax.ShapeDtypeStruct((3, ROWS, cells), F32),
            jax.ShapeDtypeStruct((1, cells), F32),
            jax.ShapeDtypeStruct((1, cells), F32),
        ),
        in_specs=[pl.BlockSpec(memory_space=pltpu.HBM)] * len(operands),
        out_specs=(anywhere, vmem, vmem),
        scratch_shapes=[pltpu.VMEM(item.shape, item.dtype) for item in operands]
        + [
            pltpu.VMEM((3, ROWS, cells), F32),
            pltpu.VMEM((ROWS, cells), F32),
            pltpu.VMEM((6, cells, cells), BF),
            pltpu.VMEM((2, ghost, cells), BF),
            pltpu.VMEM((2, cells, ghost), BF),
            pltpu.VMEM((2, MOVE, ROWS), F32),
            pltpu.VMEM((2, MOVE, ROWS), F32),
            pltpu.VMEM((2, MOVE // 2, ROWS), F32),
            pltpu.VMEM((2, MOVE // 2, ROWS), F32),
            pltpu.VMEM((2, 2, HALO, ghost), F32),
            pltpu.VMEM((2, 2, HALO, ghost), F32),
            pltpu.VMEM((ranks, 1, ROWS), F32),
            dma((len(operands),)),
            dma((3,)),
            dma((2,)),
            dma((2,)),
            dma((2,)),
            dma((2,)),
            dma((2, 2)),
            dma((2, 2)),
            dma,
            dma,
        ],
        compiler_params=pltpu.CompilerParams(
            collective_id=0, has_side_effects=True, vmem_limit_bytes=VMEM_LIMIT
        ),
    )(*operands)
    first, second, third = (basis[index, :BLOCK] for index in range(3))
    return linear * first - square * second, first - linear * second + square * third


def solution(mesh):
    both = ("curve", "group")
    shape = (mesh.shape["curve"], mesh.shape["group"])
    in_specs = (P(None, both), P(both), P(both), P(None, both), P(None, both), P(None, both))
    out_specs = (P(None, both), P(None, both))
    return jax.shard_map(
        functools.partial(body, shape),
        mesh=mesh,
        in_specs=in_specs,
        out_specs=out_specs,
        check_vma=False,
    )
```
